512 devices in a mesh: ch: 16 (over x_lo, y), row: 32 (over z, x_hi, core).
Axes of the slice: x: 4 (x_hi: 2, x_lo: 2; x = x_hi * 2 + x_lo), y: 8, z: 8, core: 2. Of those that a mesh axis runs over, the one named last changes fastest.
Arguments:
- latent: bfloat16 [512, 32, 1280], P('row', None, 'ch'), may hold values from -50 to 50
- timestep: int32 [16], replicated, may hold values from 0 to 999
- norm_gain_a: float32 [1280], P('ch'), may hold values from 0.1 to 1.9
- conv_weight_a: bfloat16 [1280, 3, 3, 1280], P('ch'), may hold values from -0.0546875 to 0.0546875
- time_weight: bfloat16 [320, 1280], P(None, 'ch'), may hold values from -0.3125 to 0.3125
- norm_gain_b: float32 [1280], P('ch'), may hold values from 0.1 to 1.9
- conv_weight_b: bfloat16 [1280, 3, 3, 1280], P('ch'), may hold values from -0.0546875 to 0.0546875
- norm_gain_c: float32 [1280], P('ch'), may hold values from 0.1 to 1.9
- w_query: bfloat16 [1024, 1280], P('ch'), may hold values from -4 to 4
- w_key: bfloat16 [1024, 1280], P('ch'), may hold values from -4 to 4
- w_value: bfloat16 [1024, 1280], P('ch'), may hold values from -0.3125 to 0.3125
- w_out: bfloat16 [1280, 1024], P('ch'), may hold values from -0.1875 to 0.1875
Outputs:
- result: bfloat16 [512, 32, 1280], P('row', None, 'ch')
The draws below stay inside these ranges and needn't reach their ends.
All inputs are finite; a program needn't handle non-finite values.
Results may differ from the reference program's by a relative error of at most 0.017.
Values may be sent and summed in bfloat16 or wider, within the bound.
No kernel may reach another device: no remote copies, remote signals or barrier semaphores. Data moves between devices by JAX's collectives and lax.ppermute only.
A program may use at most 64 MiB of HBM per device.

```python
import math
import jax
import jax.numpy as jnp
from jax import lax

C = 1280
GROUPS = 32
HEAD_DIM = 64
TDIM = 320
HEADS = 16
H = 32
W = 32
IMGS = 16
ROWS = 512


def draw_latent(key, part):
    first, second, third = jax.random.split(key, 3)
    row_place = (jnp.arange(ROWS) % H).astype(jnp.float32)
    rising = 0.6 * (1.0 + 2.0 * row_place / (H - 1))
    row_scale = rising * jnp.exp(jax.random.uniform(first, (ROWS,), minval=-0.22, maxval=0.22))
    chan_scale = jnp.exp(jax.random.uniform(second, (C,), minval=math.log(0.3), maxval=math.log(3.0)))
    base = jax.random.truncated_normal(third, -4.0, 4.0, (ROWS, W, C))
    value = base * row_scale[:, None, None] * chan_scale[None, None, :]
    return jnp.clip(value, -50.0, 50.0).astype(jnp.bfloat16)


def projection_base(key, salt):
    return jax.random.normal(jax.random.fold_in(key, salt), (HEADS * HEAD_DIM, C)) / math.sqrt(C)


def draw_w_query(key, part):
    return jnp.clip(projection_base(key, 11), -4.0, 4.0).astype(jnp.bfloat16)


def draw_w_key(key, part):
    strength = jnp.exp(jax.random.uniform(jax.random.fold_in(key, 14), (HEADS,), minval=math.log(3.0), maxval=math.log(8.0)))
    value = jnp.repeat(strength, HEAD_DIM)[:, None] * projection_base(key, 12)
    return jnp.clip(value, -4.0, 4.0).astype(jnp.bfloat16)


def plant(array, key, least, top_value):
    longest = array.shape.index(max(array.shape))
    spots = []
    for shift in (0, 1):
        where = [jax.random.randint(jax.random.fold_in(key, axis), (), 0, length) for axis, length in enumerate(array.shape)]
        where[longest] = (where[longest] + shift) % array.shape[longest]
        spots.append(tuple(where))
    return array.at[spots[0]].set(least).at[spots[1]].set(top_value)


def level_of(rng, shape, cuts, least, top_value):
    level = 1.0
    for axis_at, blocks in cuts:
        draws = jax.random.uniform(jax.random.fold_in(jax.random.fold_in(rng, 6), axis_at), (blocks,), jnp.float32, least / len(cuts), top_value / len(cuts))
        level = level * jnp.repeat(jnp.exp(draws), shape[axis_at] // blocks).reshape((-1,) + (1,) * (len(shape) - 1 - axis_at))
    return level


def scatter_about(own_key, shape, deviation, limit, shards=(), kind=jnp.bfloat16):
    level = level_of(own_key, shape, shards, -0.22, 0.18) if shards else 1.0
    array = jax.random.normal(own_key, shape, jnp.float32) * deviation * level
    return jnp.minimum(jnp.maximum(array, -limit), limit).astype(kind)


def setup_inputs(seed: int = 0) -> dict:
    seeds = jax.random.split(jax.random.key(seed), 13)
    return {
        "latent": draw_latent(jax.random.fold_in(seeds[12], 71), 0),
        "timestep": plant(jax.random.randint(seeds[1], (IMGS,), 0, 1000), jax.random.fold_in(seeds[1], 1), 0, 999).astype(jnp.int32),
        "norm_gain_a": jnp.clip(1.0 + 0.18 * jax.random.normal(seeds[2], (C,), jnp.float32), 0.1, 1.9),
        "conv_weight_a": scatter_about(seeds[3], (C, 3, 3, C), (9 * C) ** -0.5, 0.0546875, ((0, 16),)),
        "time_weight": scatter_about(seeds[4], (TDIM, C), TDIM ** -0.5, 0.3125, ((1, 16),)),
        "norm_gain_b": jnp.clip(1.0 + 0.18 * jax.random.normal(seeds[5], (C,), jnp.float32), 0.1, 1.9),
        "conv_weight_b": scatter_about(seeds[6], (C, 3, 3, C), (9 * C) ** -0.5, 0.0546875, ((0, 16),)),
        "norm_gain_c": jnp.clip(1.0 + 0.18 * jax.random.normal(seeds[7], (C,), jnp.float32), 0.1, 1.9),
        "w_query": draw_w_query(jax.random.fold_in(seeds[12], 71), 0),
        "w_key": draw_w_key(jax.random.fold_in(seeds[12], 71), 0),
        "w_value": scatter_about(seeds[10], (HEADS * HEAD_DIM, C), (C // 4) ** -0.5, 0.3125, ((0, 16),)),
        "w_out": scatter_about(seeds[11], (C, HEADS * HEAD_DIM), (HEADS * HEAD_DIM) ** -0.5, 0.1875, ((0, 16),)),
    }


eps_value = 1e-06

def group_norm(value, gain):
    members = float(H * W * (C // GROUPS))
    flat = value.reshape(value.shape[0], H * W, GROUPS, C // GROUPS)
    mean = lax.optimization_barrier(jnp.sum(flat, axis=(1, 3))) / members
    spread = lax.optimization_barrier(jnp.sum(flat * flat, axis=(1, 3))) / members - mean * mean
    scaled = (flat - mean[:, None, :, None]) * lax.rsqrt(spread + eps_value)[:, None, :, None]
    return scaled.reshape(value.shape) * gain

def convolve(active, weight):
    kernel = jnp.transpose(weight, (1, 2, 3, 0))
    return lax.conv_general_dilated(active, kernel, (1, 1), 'SAME', dimension_numbers=('NHWC', 'HWIO', 'NHWC'), preferred_element_type=jnp.float32)

def right_product(left, weight):
    return lax.dot_general(left, weight, (((1,), (1,)), ((), ())), preferred_element_type=jnp.float32)

def reference(latent, timestep, norm_gain_a, conv_weight_a, time_weight, norm_gain_b, conv_weight_b, norm_gain_c, w_query, w_key, w_value, w_out):
    source = latent.reshape(IMGS, H, W, C).astype(jnp.float32)
    active_a = jax.nn.silu(group_norm(source, norm_gain_a)).astype(jnp.bfloat16)
    half = TDIM // 2
    freqs = jnp.exp(-math.log(10000.0) * jnp.arange(half, dtype=jnp.float32) / half)
    angles = timestep.astype(jnp.float32)[:, None] * freqs[None, :]
    sinus = jnp.concatenate([jnp.cos(angles), jnp.sin(angles)], axis=1).astype(jnp.bfloat16)
    time_add = jax.nn.silu(jnp.dot(sinus, time_weight, preferred_element_type=jnp.float32))
    hidden_a = convolve(active_a, conv_weight_a) + time_add[:, None, None, :]
    active_b = jax.nn.silu(group_norm(hidden_a, norm_gain_b)).astype(jnp.bfloat16)
    hidden_b = source + convolve(active_b, conv_weight_b)
    normed = group_norm(hidden_b, norm_gain_c).astype(jnp.bfloat16).reshape(IMGS, H * W, C)
    scale = 1.0 / math.sqrt(HEAD_DIM)

    def attend(tokens_in):
        query = right_product(tokens_in, w_query).astype(jnp.bfloat16)
        keyed = right_product(tokens_in, w_key).astype(jnp.bfloat16)
        valued = right_product(tokens_in, w_value).astype(jnp.bfloat16)
        query, keyed, valued = lax.optimization_barrier((query, keyed, valued))
        query_heads = query.astype(jnp.float32).reshape(H * W, HEADS, HEAD_DIM)
        key_heads = keyed.astype(jnp.float32).reshape(H * W, HEADS, HEAD_DIM)
        value_heads = valued.astype(jnp.float32).reshape(H * W, HEADS, HEAD_DIM)
        scores = jnp.einsum('qhd,khd->hqk', query_heads, key_heads) * scale
        weights = jax.nn.softmax(scores, axis=-1).astype(jnp.bfloat16)
        weights = lax.optimization_barrier(weights)
        heads_out = jnp.einsum('hqk,khd->qhd', weights.astype(jnp.float32), value_heads)
        return heads_out.astype(jnp.bfloat16).reshape(H * W, HEADS * HEAD_DIM)
    heads_out = lax.map(attend, normed).reshape(IMGS * H * W, HEADS * HEAD_DIM)
    projected = right_product(heads_out, w_out)
    total = hidden_b.reshape(IMGS * H * W, C) + projected
    return total.reshape(ROWS, W, C).astype(jnp.bfloat16)
```

```python
import functools
import math

import jax
import jax.numpy as jnp
from jax import lax
from jax.experimental import pallas as pl
from jax.experimental.pallas import tpu as pltpu
from jax.sharding import PartitionSpec as P

C = 1280
GROUPS = 32
HEAD_DIM = 64
TDIM = 320
H = 32
W = 32
WIDE = C // GROUPS
MEMBERS = float(H * W * WIDE)
EPS = 1e-06
F32 = jnp.float32
BF16 = jnp.bfloat16

VM = pl.BlockSpec(memory_space=pltpu.VMEM)
SM = pl.BlockSpec(memory_space=pltpu.SMEM)


def call(kernel, outs, specs, scratch=()):
    return pl.pallas_call(
        kernel,
        out_shape=[jax.ShapeDtypeStruct(s, d) for s, d in outs],
        in_specs=specs,
        out_specs=[VM] * len(outs),
        scratch_shapes=list(scratch),
    )


def swapped(value):
    pairs = [(source, source ^ 1) for source in range(lax.axis_size("row"))]
    return lax.ppermute(value, "row", pairs)


def collect(block):
    peers = lax.axis_size("ch")
    pieces = jnp.broadcast_to(block[None], (peers, *block.shape))
    pieces = lax.all_to_all(pieces, "ch", 0, 0, tiled=True)
    return pieces.reshape(peers * block.shape[0], block.shape[1])


def lanes(shape):
    return lax.broadcasted_iota(jnp.int32, shape, 1)


def silu(u):
    return u / (1.0 + jnp.exp(-u))


def normalised(value, total, squares, gain):
    pieces = []
    for first in range(0, value.shape[0], WIDE):
        rows = slice(first, first + WIDE)
        mean = jnp.sum(total[rows], axis=0, keepdims=True) / MEMBERS
        spread = jnp.sum(squares[rows], axis=0, keepdims=True) / MEMBERS - mean * mean
        scale = lax.rsqrt(spread + EPS) * gain[rows]
        pieces.append((value[rows] - mean) * scale)
    return jnp.concatenate(pieces, axis=0)


def enter_kernel(latent_ref, turned_ref, sums_ref):
    value = latent_ref[...].astype(F32).T
    turned_ref[...] = value
    lane = lanes(sums_ref.shape)
    total = jnp.sum(value, axis=1, keepdims=True)
    squares = jnp.sum(value * value, axis=1, keepdims=True)
    sums_ref[...] = jnp.where(lane == 0, total, jnp.where(lane == 1, squares, 0.0))


def first_kernel(turned_ref, own_ref, peer_ref, gain_ref, active_ref):
    sums = own_ref[...] + peer_ref[...]
    value = normalised(turned_ref[...], sums[:, 0:1], sums[:, 1:2], gain_ref[...])
    active_ref[...] = silu(value).astype(BF16)


def conv_kernel(place_ref, weight_ref, full_ref, base_ref, part_ref, note_ref):
    count, tokens = part_ref.shape
    upper = place_ref[0] == 0
    token = lanes((count, tokens))
    column = token % W
    full = full_ref[...]
    combined = []
    for dy in range(3):
        rows = weight_ref[dy * 3 * count : (dy + 1) * 3 * count, :]
        taps = jnp.dot(rows, full, preferred_element_type=F32)
        left = pltpu.roll(taps[:count], 1, 1)
        right = pltpu.roll(taps[2 * count :], tokens - 1, 1)
        combined.append(
            taps[count : 2 * count]
            + jnp.where(column == 0, 0.0, left)
            + jnp.where(column == W - 1, 0.0, right)
        )
    above, middle, below = combined
    part = (
        base_ref[...]
        + middle
        + jnp.where(token < W, 0.0, pltpu.roll(above, W, 1))
        + jnp.where(token >= tokens - W, 0.0, pltpu.roll(below, tokens - W, 1))
    )
    part_ref[...] = part
    first = jnp.where(upper, 0, W)
    whole = jnp.logical_and(token >= first, token < first + tokens - W)
    kept = jnp.where(whole, part, 0.0)
    total = jnp.sum(kept, axis=1, keepdims=True)
    squares = jnp.sum(kept * kept, axis=1, keepdims=True)
    last = slice(tokens - 128, tokens)
    edge = jnp.where(upper, pltpu.roll(part[:, last], W, 1), part[:, :128])
    push = jnp.where(upper, pltpu.roll(above[:, last], 2 * W, 1), pltpu.roll(below[:, :128], W, 1))
    lane = lanes((count, 128))
    note = jnp.where(lane < W, edge, jnp.where(lane < 2 * W, push, 0.0))
    note_ref[...] = jnp.where(lane == 2 * W, total, jnp.where(lane == 2 * W + 1, squares, note))


def finish_kernel(place_ref, part_ref, own_ref, peer_ref, gain_ref, *outs, act):
    count, tokens = part_ref.shape
    upper = place_ref[0] == 0
    own, peer = own_ref[...], peer_ref[...]
    lane = lanes((count, 128))
    top = jnp.where(lane < jnp.where(upper, 0, W), pltpu.roll(peer, 128 - W, 1), 0.0)
    low = jnp.where(lane >= jnp.where(upper, 128 - W, 128), pltpu.roll(peer, 2 * W, 1), 0.0)
    part = part_ref[...]
    value = jnp.concatenate(
        [part[:, :128] + top, part[:, 128 : tokens - 128], part[:, tokens - 128 :] + low], axis=1
    )
    other = jnp.where(lane < W, peer + pltpu.roll(own, 128 - W, 1), 0.0)
    total = (
        jnp.sum(value, axis=1, keepdims=True)
        + jnp.sum(other, axis=1, keepdims=True)
        + peer[:, 2 * W : 2 * W + 1]
    )
    squares = (
        jnp.sum(value * value, axis=1, keepdims=True)
        + jnp.sum(other * other, axis=1, keepdims=True)
        + peer[:, 2 * W + 1 : 2 * W + 2]
    )
    result = normalised(value, total, squares, gain_ref[...])
    if act:
        outs[0][...] = silu(result).astype(BF16)
    else:
        outs[0][...] = result.astype(BF16)
        outs[1][...] = value


def project_kernel(query_ref, key_ref, value_ref, full_ref, q_ref, kv_ref, stack_ref):
    inner = query_ref.shape[0]
    stack_ref[:inner] = query_ref[...]
    stack_ref[inner : 2 * inner] = key_ref[...]
    stack_ref[2 * inner :] = value_ref[...]
    mixed = jnp.dot(stack_ref[...], full_ref[...], preferred_element_type=F32).astype(BF16)
    q_ref[...] = mixed[:inner]
    kv_ref[...] = mixed[inner:]


def attend_kernel(q_ref, own_ref, peer_ref, out_ref):
    inner = q_ref.shape[0]
    keys = jnp.concatenate([own_ref[:inner], peer_ref[:inner]], axis=1)
    values = jnp.concatenate([own_ref[inner:], peer_ref[inner:]], axis=1)
    scores = lax.dot_general(
        keys, q_ref[...], (((0,), (0,)), ((), ())), preferred_element_type=F32
    ) * (1.0 / math.sqrt(HEAD_DIM))
    raised = jnp.exp(scores - jnp.max(scores, axis=0, keepdims=True))
    weights = (raised * (1.0 / jnp.sum(raised, axis=0, keepdims=True))).astype(BF16)
    out_ref[...] = jnp.dot(values, weights, preferred_element_type=F32).astype(BF16)


def leave_kernel(weight_ref, full_ref, hidden_ref, result_ref):
    total = hidden_ref[...] + jnp.dot(weight_ref[...], full_ref[...], preferred_element_type=F32)
    result_ref[...] = total.T.astype(BF16)


def body(
    latent,
    timestep,
    norm_gain_a,
    conv_weight_a,
    time_weight,
    norm_gain_b,
    conv_weight_b,
    norm_gain_c,
    w_query,
    w_key,
    w_value,
    w_out,
):
    rows, width, count = latent.shape
    tokens = rows * width
    span = H // rows
    place = lax.axis_index("row")
    within = (place % span).astype(jnp.int32).reshape(1)
    image_id = place // span
    inner = w_query.shape[0]

    def tall(weight):
        return jnp.transpose(weight, (1, 2, 0, 3)).reshape(9 * count, C)

    def column(gain):
        return gain.reshape(count, 1)

    step_value = jnp.sum(jnp.where(jnp.arange(timestep.shape[0]) == image_id, timestep, 0)).astype(F32)
    half = TDIM // 2
    freqs = jnp.exp(-math.log(10000.0) * jnp.arange(half, dtype=F32) / half)
    angles = step_value * freqs
    sinus = jnp.concatenate([jnp.cos(angles), jnp.sin(angles)])[None, :].astype(BF16)
    time_add = jax.nn.silu(jnp.dot(sinus, time_weight, preferred_element_type=F32)).reshape(count, 1)

    field = ((count, tokens), F32)
    note = ((count, 128), F32)
    active = ((count, tokens), BF16)

    turned, sums = call(enter_kernel, [field, note], [VM])(latent.reshape(tokens, count))
    (active_a,) = call(first_kernel, [active], [VM] * 4)(turned, sums, swapped(sums), column(norm_gain_a))

    conv = call(conv_kernel, [field, note], [SM, VM, VM, VM])
    part, own = conv(within, tall(conv_weight_a), collect(active_a), time_add)
    (active_b,) = call(functools.partial(finish_kernel, act=True), [active], [SM] + [VM] * 4)(
        within, part, own, swapped(own), column(norm_gain_b)
    )
    part, own = conv(within, tall(conv_weight_b), collect(active_b), turned)
    normed, hidden_b = call(functools.partial(finish_kernel, act=False), [active, field], [SM] + [VM] * 4)(
        within, part, own, swapped(own), column(norm_gain_c)
    )
    query, key_value = call(
        project_kernel,
        [((inner, tokens), BF16), ((2 * inner, tokens), BF16)],
        [VM] * 4,
        [pltpu.VMEM((3 * inner, C), BF16)],
    )(w_query, w_key, w_value, collect(normed))
    (heads_out,) = call(attend_kernel, [((inner, tokens), BF16)], [VM] * 3)(
        query, key_value, swapped(key_value)
    )
    (result,) = call(leave_kernel, [((tokens, count), BF16)], [VM] * 3)(w_out, collect(heads_out), hidden_b)
    return result.reshape(rows, width, count)


def solution(mesh):
    return jax.shard_map(
        body,
        mesh=mesh,
        in_specs=(
            P("row", None, "ch"),
            P(),
            P("ch"),
            P("ch", None, None, None),
            P(None, "ch"),
            P("ch"),
            P("ch", None, None, None),
            P("ch"),
            P("ch", None),
            P("ch", None),
            P("ch", None),
            P("ch", None),
        ),
        out_specs=P("row", None, "ch"),
        check_vma=False,
    )
```

```python
import functools
import math

import jax
import jax.numpy as jnp
from jax import lax
from jax.experimental import pallas as pl
from jax.experimental.pallas import tpu as pltpu
from jax.sharding import PartitionSpec as P

C = 1280
GROUPS = 32
HEAD_DIM = 64
TDIM = 320
H = 32
W = 32
WIDE = C // GROUPS
MEMBERS = float(H * W * WIDE)
EPS = 1e-06
F32 = jnp.float32
BF16 = jnp.bfloat16

VM = pl.BlockSpec(memory_space=pltpu.VMEM)
SM = pl.BlockSpec(memory_space=pltpu.SMEM)


def call(kernel, outs, specs, scratch=()):
    return pl.pallas_call(
        kernel,
        out_shape=[jax.ShapeDtypeStruct(s, d) for s, d in outs],
        in_specs=specs,
        out_specs=[VM] * len(outs),
        scratch_shapes=list(scratch),
    )


def device(ch, row):
    return ch * lax.axis_size("row") + row


def core_pairs():
    rows, chs = lax.axis_size("row"), lax.axis_size("ch")
    return [(device(k, r), device(k, r ^ 1)) for k in range(chs) for r in range(rows)]


def swapped(value):
    return lax.ppermute(value, ("ch", "row"), core_pairs())


def crossed(value):
    chs = lax.axis_size("ch")
    return lax.ppermute(value, "ch", [(k, (k + chs // 2) % chs) for k in range(chs)])


def from_beside(value):
    rows, chs = lax.axis_size("row"), lax.axis_size("ch")
    wide = 2 if rows % 4 == 0 else 1
    pairs = []
    for k in range(chs):
        for r in range(rows):
            core, high, rest = r % 2, r // 2 % wide, r // (2 * wide)
            x = (2 * high + k // (chs // 2) + (1 if core == 0 else -1)) % (2 * wide)
            source = device(x % 2 * (chs // 2) + k % (chs // 2), (rest * wide + x // 2) * 2 + core)
            pairs.append((source, device(k, r)))
    return lax.ppermute(value, ("ch", "row"), pairs)


def copies(block, count):
    return jnp.broadcast_to(block[None], (count, *block.shape))


def column_collect(block):
    half = lax.axis_size("ch") // 2
    groups = [list(range(half)), list(range(half, 2 * half))]
    return lax.all_to_all(copies(block, half), "ch", 0, 0, tiled=True, axis_index_groups=groups)


def image_collect(block):
    rows, half = lax.axis_size("row"), lax.axis_size("ch") // 2
    groups = [
        [device(k, r), device(k + half, r), device(k + half, r + 1), device(k, r + 1)]
        for r in range(0, rows, 2)
        for k in range(half)
    ]
    return lax.all_to_all(copies(block, 4), ("ch", "row"), 0, 0, tiled=True, axis_index_groups=groups)


def lanes(shape):
    return lax.broadcasted_iota(jnp.int32, shape, 1)


def silu(u):
    return u / (1.0 + jnp.exp(-u))


def scaled(value, total, squares, gain):
    mean = total / MEMBERS
    spread = squares / MEMBERS - mean * mean
    return (value - mean) * (lax.rsqrt(spread + EPS) * gain)


def by_group(per_channel):
    return [
        jnp.sum(per_channel[first : first + WIDE], axis=0, keepdims=True)
        for first in range(0, per_channel.shape[0], WIDE)
    ]


def enter_kernel(place_ref, latent_ref, turned_ref, keep_ref, send_ref, sums_ref):
    value = latent_ref[...].astype(F32).T
    turned_ref[...] = value
    half = value.shape[1] // 2
    first = place_ref[2] == 0
    keep_ref[...] = jnp.where(first, value[:, :half], value[:, half:])
    send_ref[...] = jnp.where(first, value[:, half:], value[:, :half])
    lane = lanes(sums_ref.shape)
    total = jnp.sum(value, axis=1, keepdims=True)
    squares = jnp.sum(value * value, axis=1, keepdims=True)
    sums_ref[...] = jnp.where(lane == 0, total, jnp.where(lane == 1, squares, 0.0))


def first_kernel(place_ref, turned_ref, own_ref, peer_ref, gain_ref, active_ref):
    sums = own_ref[...] + peer_ref[...]
    totals, squares = by_group(sums[:, 0:1]), by_group(sums[:, 1:2])
    pieces = []
    for group in range(len(totals)):
        rows = slice(group * WIDE, (group + 1) * WIDE)
        pieces.append(scaled(turned_ref[rows], totals[group], squares[group], gain_ref[rows]))
    value = silu(jnp.concatenate(pieces, axis=0)).astype(BF16)
    half = value.shape[1] // 2
    core = place_ref[1]
    active_ref[core] = value[:, :half]
    active_ref[1 - core] = value[:, half:]


def gather_into(full_ref, whole_ref):
    if len(full_ref.shape) == 3:
        whole_ref[...] = full_ref[...].reshape(whole_ref.shape)
        return
    peers, _, count, _ = full_ref.shape
    for side in range(2):
        for peer in range(peers):
            at = (side * peers + peer) * count
            whole_ref[at : at + count] = full_ref[peer, side]


def both(core, own, got, other, whole_ref):
    depth = got.shape[1]
    near = whole_ref[pl.ds(pl.multiple_of(core * depth, 128), depth), :]
    far = whole_ref[pl.ds(pl.multiple_of((1 - core) * depth, 128), depth), :]
    return (
        jnp.dot(own, whole_ref[...], preferred_element_type=F32),
        jnp.dot(got, near, preferred_element_type=F32) + jnp.dot(other, far, preferred_element_type=F32),
    )


def conv_kernel(place_ref, own_ref, got_ref, other_ref, full_ref, base_ref, far_ref, part_ref, note_ref, whole_ref, *, at):
    _, count, tokens = part_ref.shape
    side, core, quarter = place_ref[0], place_ref[1], place_ref[3]
    token = lanes((count, tokens))
    column = token % W
    lane = lanes((count, 128))
    begin = jnp.where(quarter > 0, W, 0)
    end = jnp.where(quarter < 3, tokens - W, tokens)
    gather_into(full_ref, whole_ref)
    taps = both(core, own_ref[...], got_ref[: 9 * count], other_ref[: 9 * count], whole_ref)
    bases = base_ref[...], far_ref[:, at]
    extra = jnp.zeros((16, 128), F32)
    spot = lanes((16, 128))
    for which in range(2):
        here = side if which == 0 else 1 - side
        combined = []
        for dy in range(3):
            left, middle, right = (
                taps[which][(3 * dy + dx) * count : (3 * dy + dx + 1) * count] for dx in range(3)
            )
            combined.append(
                middle
                + jnp.where(column == 0, 0.0, pltpu.roll(left, 1, 1))
                + jnp.where(column == W - 1, 0.0, pltpu.roll(right, tokens - 1, 1))
            )
        above, middle, below = combined
        part = (
            bases[which]
            + middle
            + jnp.where(token < W, 0.0, pltpu.roll(above, W, 1))
            + jnp.where(token >= tokens - W, 0.0, pltpu.roll(below, tokens - W, 1))
        )
        part_ref[here] = part
        kept = jnp.where(jnp.logical_and(token >= begin, token < end), part, 0.0)
        totals = by_group(jnp.sum(kept, axis=1, keepdims=True))
        squares = by_group(jnp.sum(kept * kept, axis=1, keepdims=True))
        bottom = pltpu.roll(part[:, tokens - 128 :], 2 * W, 1)
        up = pltpu.roll(below[:, :128], 2 * W, 1)
        note = jnp.where(lane < W, part[:, :128], jnp.where(lane < 2 * W, bottom, jnp.where(lane < 3 * W, up, above[:, tokens - 128 :])))
        note_ref[pl.ds(pl.multiple_of(here * count, 16), count), :] = note.astype(BF16)
        for group in range(len(totals)):
            for kind, value in enumerate((totals[group], squares[group])):
                for piece in range(3):
                    rounded = value.astype(BF16).astype(F32)
                    index = (here * len(totals) + group) * 6 + kind * 3 + piece
                    extra = jnp.where(spot == index, rounded, extra)
                    value = value - rounded
    note_ref[2 * count :, :] = extra.astype(BF16)


def finish_kernel(place_ref, part_ref, notes_ref, gains_ref, *outs, act, lane_of):
    _, count, tokens = part_ref.shape
    quarter = place_ref[3]
    lane = lanes((count, 128))
    sums = notes_ref[0, 2 * count :].astype(F32)
    for place in range(1, 4):
        sums = sums + notes_ref[place, 2 * count :].astype(F32)
    before = jnp.maximum(quarter - 1, 0)
    after = jnp.minimum(quarter + 1, 3)
    for side in range(2):
        rows = slice(side * count, (side + 1) * count)
        notes = [notes_ref[place, rows].astype(F32) for place in range(4)]
        total = jnp.zeros((count, 1), F32)
        squares = jnp.zeros((count, 1), F32)
        for low in range(3):
            one, two = notes[low], notes[low + 1]
            edges = jnp.where(
                lane < W,
                two + pltpu.roll(one, W, 1),
                jnp.where(lane < 2 * W, one + pltpu.roll(two, 128 - W, 1), 0.0),
            )
            total = total + jnp.sum(edges, axis=1, keepdims=True)
            squares = squares + jnp.sum(edges * edges, axis=1, keepdims=True)
        top = pltpu.roll(notes_ref[before, rows].astype(F32), W, 1)
        low = pltpu.roll(notes_ref[after, rows].astype(F32), W, 1)
        part = part_ref[side]
        value = jnp.concatenate(
            [
                part[:, :128] + jnp.where(lane < jnp.where(quarter > 0, W, 0), top, 0.0),
                part[:, tokens - 128 :] + jnp.where(lane >= jnp.where(quarter < 3, 128 - W, 128), low, 0.0),
            ],
            axis=1,
        )
        totals, squared = by_group(total), by_group(squares)
        gain = gains_ref[side][:, lane_of : lane_of + 1]
        pieces = []
        for group in range(len(totals)):
            first = (side * len(totals) + group) * 6
            whole = totals[group] + jnp.sum(sums[0:1, first : first + 3], axis=1, keepdims=True)
            whole_squares = squared[group] + jnp.sum(sums[0:1, first + 3 : first + 6], axis=1, keepdims=True)
            span = slice(group * WIDE, (group + 1) * WIDE)
            pieces.append(scaled(value[span], whole, whole_squares, gain[span]))
        result = jnp.concatenate(pieces, axis=0)
        if act:
            outs[0][side] = silu(result).astype(BF16)
        else:
            outs[0][side] = result.astype(BF16)
            outs[1][side] = value


def project_kernel(place_ref, query_ref, key_ref, value_ref, got_ref, other_ref, full_ref, q_ref, kv_ref, whole_ref, stack_ref, *, at):
    inner = query_ref.shape[0]
    side, core = place_ref[0], place_ref[1]
    stack_ref[:inner] = query_ref[...]
    stack_ref[inner : 2 * inner] = key_ref[...]
    stack_ref[2 * inner :] = value_ref[...]
    gather_into(full_ref, whole_ref)
    rows = slice(at, at + 3 * inner)
    mixed = both(core, stack_ref[...], got_ref[rows], other_ref[rows], whole_ref)
    for which in range(2):
        here = side if which == 0 else 1 - side
        q_ref[here] = mixed[which][:inner].astype(BF16)
        kv_ref[here] = mixed[which][inner:].astype(BF16)


def attend_kernel(q_ref, pairs_ref, out_ref):
    inner = q_ref.shape[1]
    for head in range(2):
        keys = jnp.concatenate([pairs_ref[place, head, :inner] for place in range(4)], axis=1)
        values = jnp.concatenate([pairs_ref[place, head, inner:] for place in range(4)], axis=1)
        scores = lax.dot_general(
            keys, q_ref[head], (((0,), (0,)), ((), ())), preferred_element_type=F32
        ) * (1.0 / math.sqrt(HEAD_DIM))
        raised = jnp.exp(scores - jnp.max(scores, axis=0, keepdims=True))
        weights = (raised * (1.0 / jnp.sum(raised, axis=0, keepdims=True))).astype(BF16)
        out_ref[head] = jnp.dot(values, weights, preferred_element_type=F32).astype(BF16)


def leave_kernel(place_ref, weight_ref, got_ref, other_ref, full_ref, hidden_ref, keep_ref, send_ref, whole_ref, *, at):
    count, depth = weight_ref.shape
    side, core = place_ref[0], place_ref[1]
    gather_into(full_ref, whole_ref)
    got, other = (ref[at : at + count, : depth // 2] for ref in (got_ref, other_ref))
    mine, theirs = both(core, weight_ref[...], got, other, whole_ref)
    keep_ref[...] = (hidden_ref[side] + mine).astype(BF16)
    send_ref[...] = (hidden_ref[1 - side] + theirs).astype(BF16)


def last_kernel(place_ref, keep_ref, peer_ref, result_ref):
    span = keep_ref.shape[1]
    part = place_ref[2]
    for ref, at in ((keep_ref, part), (peer_ref, 1 - part)):
        result_ref[pl.ds(pl.multiple_of(at * span, 16), span), :] = ref[...].astype(F32).T.astype(BF16)


def body(
    latent,
    timestep,
    norm_gain_a,
    conv_weight_a,
    time_weight,
    norm_gain_b,
    conv_weight_b,
    norm_gain_c,
    w_query,
    w_key,
    w_value,
    w_out,
):
    rows, width, count = latent.shape
    tokens = rows * width
    share = tokens // 2
    chs = lax.axis_size("ch")
    channel, place = lax.axis_index("ch"), lax.axis_index("row")
    side, core = channel // (chs // 2), place % 2
    part = side ^ core
    where = jnp.stack([side, core, part, 2 * core + part]).astype(jnp.int32)
    image_id = place // 2
    inner = w_query.shape[0]

    def tall(weight):
        return jnp.transpose(weight, (1, 2, 0, 3)).reshape(9 * count, C)

    def halved(weight):
        depth = weight.shape[1] // 2
        return lax.dynamic_slice_in_dim(weight, core * depth, depth, axis=1)

    step_value = jnp.sum(jnp.where(jnp.arange(timestep.shape[0]) == image_id, timestep, 0)).astype(F32)
    half = TDIM // 2
    freqs = jnp.exp(-math.log(10000.0) * jnp.arange(half, dtype=F32) / half)
    angles = step_value * freqs
    sinus = jnp.concatenate([jnp.cos(angles), jnp.sin(angles)])[None, :].astype(BF16)
    time_add = jax.nn.silu(jnp.dot(sinus, time_weight, preferred_element_type=F32))[0]
    vector = jnp.pad(jnp.stack([time_add, norm_gain_b, norm_gain_c], axis=1), ((0, 0), (0, 125)))

    field = ((2, count, share), F32)
    active = ((2, count, share), BF16)
    quarter = ((count, share), F32)
    note = ((2 * count + 16, 128), BF16)
    whole = pltpu.VMEM((C, share), BF16)

    turned, keep, send, sums = call(
        enter_kernel, [((count, tokens), F32), quarter, quarter, ((count, 128), F32)], [SM, VM]
    )(where, latent.reshape(tokens, count))
    (active_a,) = call(first_kernel, [active], [SM] + [VM] * 4)(
        where, turned, sums, swapped(sums), norm_gain_a.reshape(count, 1)
    )

    own_a, own_b = tall(conv_weight_a), tall(conv_weight_b)
    mail = crossed(jnp.concatenate([send, vector], axis=1))
    got_a = from_beside(halved(own_a))
    late = jnp.concatenate([w_query, w_key, w_value], axis=0)
    late_out = jnp.pad(halved(w_out), ((0, 0), (0, (C - w_out.shape[1]) // 2)))
    got_b = from_beside(jnp.concatenate([halved(own_b), halved(late), late_out], axis=0))
    theirs = mail[:, share:]
    vectors = jnp.where(side == 0, jnp.stack([vector, theirs]), jnp.stack([theirs, vector]))

    spread = jnp.broadcast_to(active_a[:, None], (2, chs // 2, count, share)).reshape(chs, count, share)
    full = lax.all_to_all(spread, "ch", 0, 0, tiled=True)
    other_a = swapped(got_a)

    def conv(full, own, got, other, base, at):
        return call(
            functools.partial(conv_kernel, at=at), [field, note], [SM] + [VM] * 6, [whole]
        )(where, own, got, other, full, base, mail)

    def finish(part, note, act, lane_of, outs):
        return call(
            functools.partial(finish_kernel, act=act, lane_of=lane_of), outs, [SM] + [VM] * 3
        )(where, part, image_collect(note), vectors)

    part_a, note_a = conv(full, own_a, got_a, other_a, vector[:, 0:1], slice(share, share + 1))
    (active_b,) = finish(part_a, note_a, True, 1, [active])
    other_b = swapped(got_b)
    part_b, note_b = conv(column_collect(active_b), own_b, got_b, other_b, keep, slice(0, share))
    normed, hidden_b = finish(part_b, note_b, False, 2, [active, field])

    query, key_value = call(
        functools.partial(project_kernel, at=9 * count),
        [((2, inner, share), BF16), ((2, 2 * inner, share), BF16)],
        [SM] + [VM] * 6,
        [whole, pltpu.VMEM((3 * inner, C), BF16)],
    )(where, w_query, w_key, w_value, got_b, other_b, column_collect(normed))
    (heads_out,) = call(attend_kernel, [((2, inner, share), BF16)], [VM] * 2)(
        query, image_collect(key_value)
    )
    kept, sent = call(
        functools.partial(leave_kernel, at=9 * count + 3 * inner),
        [((count, share), BF16)] * 2,
        [SM] + [VM] * 5,
        [pltpu.VMEM((w_out.shape[1], share), BF16)],
    )(where, w_out, got_b, other_b, column_collect(heads_out), hidden_b)
    (result,) = call(last_kernel, [((tokens, count), BF16)], [SM] + [VM] * 2)(where, kept, crossed(sent))
    return result.reshape(rows, width, count)


def solution(mesh):
    return jax.shard_map(
        body,
        mesh=mesh,
        in_specs=(
            P("row", None, "ch"),
            P(),
            P("ch"),
            P("ch", None, None, None),
            P(None, "ch"),
            P("ch"),
            P("ch", None, None, None),
            P("ch"),
            P("ch", None),
            P("ch", None),
            P("ch", None),
            P("ch", None),
        ),
        out_specs=P("row", None, "ch"),
        check_vma=False,
    )
```

```python
import functools
import math

import jax
import jax.numpy as jnp
from jax import lax
from jax.experimental import pallas as pl
from jax.experimental.pallas import tpu as pltpu
from jax.sharding import PartitionSpec as P

C = 1280
GROUPS = 32
HEAD_DIM = 64
TDIM = 320
H = 32
W = 32
WIDE = C // GROUPS
MEMBERS = float(H * W * WIDE)
EPS = 1e-06
F32 = jnp.float32
BF16 = jnp.bfloat16

VM = pl.BlockSpec(memory_space=pltpu.VMEM)


def call(kernel, outs, specs, scratch=()):
    return pl.pallas_call(
        kernel,
        out_shape=[jax.ShapeDtypeStruct(s, d) for s, d in outs],
        in_specs=specs,
        out_specs=[VM] * len(outs),
        scratch_shapes=list(scratch),
        compiler_params=pltpu.CompilerParams(vmem_limit_bytes=20 * 2**20),
    )


def device(ch, row):
    return ch * lax.axis_size("row") + row


def core_pairs():
    rows, chs = lax.axis_size("row"), lax.axis_size("ch")
    return [(device(k, r), device(k, r ^ 1)) for k in range(chs) for r in range(rows)]


def swapped(value):
    return lax.ppermute(value, ("ch", "row"), core_pairs())


def crossed(value):
    chs = lax.axis_size("ch")
    return lax.ppermute(value, "ch", [(k, (k + chs // 2) % chs) for k in range(chs)])


def from_beside(value):
    rows, chs = lax.axis_size("row"), lax.axis_size("ch")
    wide = 2 if rows % 4 == 0 else 1
    pairs = []
    for k in range(chs):
        for r in range(rows):
            core, high, rest = r % 2, r // 2 % wide, r // (2 * wide)
            x = (2 * high + k // (chs // 2) + (1 if core == 0 else -1)) % (2 * wide)
            source = device(x % 2 * (chs // 2) + k % (chs // 2), (rest * wide + x // 2) * 2 + core)
            pairs.append((source, device(k, r)))
    return lax.ppermute(value, ("ch", "row"), pairs)


def spot():
    side = lax.axis_index("ch") // (lax.axis_size("ch") // 2)
    core = lax.axis_index("row") % 2
    return side, core, 2 * core + (side ^ core)


def after(value, first):
    return lax.optimization_barrier((value, first))[0]


def copies(block, count):
    return jnp.broadcast_to(block[None], (count, *block.shape))


def column_copies(block):
    return copies(block, lax.axis_size("ch") // 2)


def column_collect(spread):
    half = lax.axis_size("ch") // 2
    groups = [list(range(half)), list(range(half, 2 * half))]
    return lax.all_to_all(spread, "ch", 0, 0, tiled=True, axis_index_groups=groups)


def image_collect(block):
    rows, half = lax.axis_size("row"), lax.axis_size("ch") // 2
    groups = [
        [device(k, r), device(k + half, r), device(k + half, r + 1), device(k, r + 1)]
        for r in range(0, rows, 2)
        for k in range(half)
    ]
    return lax.all_to_all(copies(block, 4), ("ch", "row"), 0, 0, tiled=True, axis_index_groups=groups)


def lanes(shape):
    return lax.broadcasted_iota(jnp.int32, shape, 1)


def silu(u):
    return u / (1.0 + jnp.exp(-u))


def scaled(value, total, squares, gain):
    mean = total / MEMBERS
    spread = squares / MEMBERS - mean * mean
    return (value - mean) * (lax.rsqrt(spread + EPS) * gain)


def by_group(per_channel):
    return [
        jnp.sum(per_channel[first : first + WIDE], axis=0, keepdims=True)
        for first in range(0, per_channel.shape[0], WIDE)
    ]


def enter_kernel(latent_ref, gain_a_ref, gain_b_ref, gain_c_ref, turned_ref, keep_ref, send_ref, sums_ref):
    side, core, _ = spot()
    value = latent_ref[...].astype(F32).T
    turned_ref[...] = value
    half = value.shape[1] // 2
    first = side == core
    keep_ref[...] = jnp.where(first, value[:, :half], value[:, half:])
    send_ref[...] = jnp.where(first, value[:, half:], value[:, :half])
    lane = lanes(sums_ref.shape)
    gains = [ref[...] for ref in (gain_a_ref, gain_b_ref, gain_c_ref)]
    gains = jnp.concatenate(gains + [jnp.zeros((5, gains[0].shape[1]), F32)], axis=0).T
    total = jnp.sum(value, axis=1, keepdims=True)
    squares = jnp.sum(value * value, axis=1, keepdims=True)
    sums = jnp.where(lane == 0, total, jnp.where(lane == 1, squares, 0.0))
    for kind in range(3):
        sums = jnp.where(lane == 2 + kind, gains[:, kind : kind + 1], sums)
    sums_ref[...] = sums


def first_kernel(turned_ref, own_ref, peer_ref, active_ref):
    _, core, _ = spot()
    sums = own_ref[...] + peer_ref[...]
    totals, squares = by_group(sums[:, 0:1]), by_group(sums[:, 1:2])
    gain = own_ref[:, 2:3]
    pieces = []
    for group in range(len(totals)):
        rows = slice(group * WIDE, (group + 1) * WIDE)
        pieces.append(scaled(turned_ref[rows], totals[group], squares[group], gain[rows]))
    value = silu(jnp.concatenate(pieces, axis=0)).astype(BF16)
    half = value.shape[1] // 2
    active_ref[core] = value[:, :half]
    active_ref[1 - core] = value[:, half:]


def mail_kernel(weight_ref, sinus_ref, own_ref, send_ref, vector_ref, mail_ref):
    product = weight_ref[...].astype(F32) * sinus_ref[...].astype(F32)
    time_add = silu(jnp.sum(product, axis=1, keepdims=True))
    lane = lanes(vector_ref.shape)
    vector = jnp.where(lane == 0, time_add, 0.0)
    for kind in range(2):
        vector = jnp.where(lane == 1 + kind, own_ref[:, 3 + kind : 4 + kind], vector)
    vector_ref[...] = vector
    share = send_ref.shape[1]
    mail_ref[:, :share] = send_ref[...]
    mail_ref[:, share:] = vector


def gather_into(full_ref, whole_ref):
    if len(full_ref.shape) == 3:
        whole_ref[...] = full_ref[...].reshape(whole_ref.shape)
        return
    peers, _, count, _ = full_ref.shape
    for side in range(2):
        for peer in range(peers):
            at = (side * peers + peer) * count
            whole_ref[at : at + count] = full_ref[peer, side]


def both(core, own, got, other, whole_ref):
    depth = got.shape[1]
    near = whole_ref[pl.ds(pl.multiple_of(core * depth, 128), depth), :]
    far = whole_ref[pl.ds(pl.multiple_of((1 - core) * depth, 128), depth), :]
    return (
        jnp.dot(own, whole_ref[...], preferred_element_type=F32),
        jnp.dot(got, near, preferred_element_type=F32) + jnp.dot(other, far, preferred_element_type=F32),
    )


def conv_kernel(own_ref, got_ref, other_ref, full_ref, base_ref, far_ref, part_ref, note_ref, whole_ref, *, near, far):
    _, count, tokens = part_ref.shape
    side, core, quarter = spot()
    token = lanes((count, tokens))
    column = token % W
    lane = lanes((count, 128))
    begin = jnp.where(quarter > 0, W, 0)
    end = jnp.where(quarter < 3, tokens - W, tokens)
    gather_into(full_ref, whole_ref)
    taps = both(core, own_ref[...], got_ref[: 9 * count], other_ref[: 9 * count], whole_ref)
    bases = base_ref[:, near], far_ref[:, far]
    extra = jnp.zeros((16, 128), F32)
    extra_lane = lanes((16, 128))
    for which in range(2):
        here = side if which == 0 else 1 - side
        combined = []
        for dy in range(3):
            left, middle, right = (
                taps[which][(3 * dy + dx) * count : (3 * dy + dx + 1) * count] for dx in range(3)
            )
            combined.append(
                middle
                + jnp.where(column == 0, 0.0, pltpu.roll(left, 1, 1))
                + jnp.where(column == W - 1, 0.0, pltpu.roll(right, tokens - 1, 1))
            )
        above, middle, below = combined
        part = (
            bases[which]
            + middle
            + jnp.where(token < W, 0.0, pltpu.roll(above, W, 1))
            + jnp.where(token >= tokens - W, 0.0, pltpu.roll(below, tokens - W, 1))
        )
        part_ref[here] = part
        kept = jnp.where(jnp.logical_and(token >= begin, token < end), part, 0.0)
        totals = by_group(jnp.sum(kept, axis=1, keepdims=True))
        squares = by_group(jnp.sum(kept * kept, axis=1, keepdims=True))
        bottom = pltpu.roll(part[:, tokens - 128 :], 2 * W, 1)
        up = pltpu.roll(below[:, :128], 2 * W, 1)
        note = jnp.where(lane < W, part[:, :128], jnp.where(lane < 2 * W, bottom, jnp.where(lane < 3 * W, up, above[:, tokens - 128 :])))
        note_ref[pl.ds(pl.multiple_of(here * count, 16), count), :] = note.astype(BF16)
        for group in range(len(totals)):
            for kind, value in enumerate((totals[group], squares[group])):
                for piece in range(3):
                    rounded = value.astype(BF16).astype(F32)
                    index = (here * len(totals) + group) * 6 + kind * 3 + piece
                    extra = jnp.where(extra_lane == index, rounded, extra)
                    value = value - rounded
    note_ref[2 * count :, :] = extra.astype(BF16)


def finish_kernel(part_ref, notes_ref, vector_ref, mail_ref, *outs, act, lane_of):
    _, count, tokens = part_ref.shape
    mine, _, quarter = spot()
    lane = lanes((count, 128))
    sums = notes_ref[0, 2 * count :].astype(F32)
    for place in range(1, 4):
        sums = sums + notes_ref[place, 2 * count :].astype(F32)
    before = jnp.maximum(quarter - 1, 0)
    after = jnp.minimum(quarter + 1, 3)
    for side in range(2):
        rows = slice(side * count, (side + 1) * count)
        notes = [notes_ref[place, rows].astype(F32) for place in range(4)]
        total = jnp.zeros((count, 1), F32)
        squares = jnp.zeros((count, 1), F32)
        for low in range(3):
            one, two = notes[low], notes[low + 1]
            edges = jnp.where(
                lane < W,
                two + pltpu.roll(one, W, 1),
                jnp.where(lane < 2 * W, one + pltpu.roll(two, 128 - W, 1), 0.0),
            )
            total = total + jnp.sum(edges, axis=1, keepdims=True)
            squares = squares + jnp.sum(edges * edges, axis=1, keepdims=True)
        top = pltpu.roll(notes_ref[before, rows].astype(F32), W, 1)
        low = pltpu.roll(notes_ref[after, rows].astype(F32), W, 1)
        part = part_ref[side]
        value = jnp.concatenate(
            [
                part[:, :128] + jnp.where(lane < jnp.where(quarter > 0, W, 0), top, 0.0),
                part[:, tokens - 128 :] + jnp.where(lane >= jnp.where(quarter < 3, 128 - W, 128), low, 0.0),
            ],
            axis=1,
        )
        totals, squared = by_group(total), by_group(squares)
        at = tokens + lane_of
        gain = jnp.where(side == mine, vector_ref[:, lane_of : lane_of + 1], mail_ref[:, at : at + 1])
        pieces = []
        for group in range(len(totals)):
            first = (side * len(totals) + group) * 6
            whole = totals[group] + jnp.sum(sums[0:1, first : first + 3], axis=1, keepdims=True)
            whole_squares = squared[group] + jnp.sum(sums[0:1, first + 3 : first + 6], axis=1, keepdims=True)
            span = slice(group * WIDE, (group + 1) * WIDE)
            pieces.append(scaled(value[span], whole, whole_squares, gain[span]))
        result = jnp.concatenate(pieces, axis=0)
        if act:
            outs[0][side] = silu(result).astype(BF16)
        else:
            outs[0][side] = result.astype(BF16)
            outs[1][side] = value


def project_kernel(*refs, at):
    *own_refs, got_ref, other_ref, full_ref, out_ref, whole_ref, stack_ref = refs
    inner = own_refs[0].shape[0]
    side, core, _ = spot()
    for index, ref in enumerate(own_refs):
        stack_ref[index * inner : (index + 1) * inner] = ref[...]
    gather_into(full_ref, whole_ref)
    rows = slice(at, at + len(own_refs) * inner)
    mixed = both(core, stack_ref[...], got_ref[rows], other_ref[rows], whole_ref)
    for which in range(2):
        out_ref[side if which == 0 else 1 - side] = mixed[which].astype(BF16)


def attend_kernel(q_ref, pairs_ref, out_ref):
    inner = q_ref.shape[1]
    for head in range(2):
        keys = jnp.concatenate([pairs_ref[place, head, :inner] for place in range(4)], axis=1)
        values = jnp.concatenate([pairs_ref[place, head, inner:] for place in range(4)], axis=1)
        scores = lax.dot_general(
            keys, q_ref[head], (((0,), (0,)), ((), ())), preferred_element_type=F32
        ) * (1.0 / math.sqrt(HEAD_DIM))
        raised = jnp.exp(scores - jnp.max(scores, axis=0, keepdims=True))
        weights = (raised * (1.0 / jnp.sum(raised, axis=0, keepdims=True))).astype(BF16)
        out_ref[head] = jnp.dot(values, weights, preferred_element_type=F32).astype(BF16)


def leave_kernel(weight_ref, got_ref, other_ref, full_ref, hidden_ref, keep_ref, send_ref, whole_ref, *, at):
    count, depth = weight_ref.shape
    side, core, _ = spot()
    gather_into(full_ref, whole_ref)
    got, other = (ref[at : at + count, : depth // 2] for ref in (got_ref, other_ref))
    mine, theirs = both(core, weight_ref[...], got, other, whole_ref)
    keep_ref[...] = (hidden_ref[side] + mine).astype(BF16)
    send_ref[...] = (hidden_ref[1 - side] + theirs).astype(BF16)


def last_kernel(keep_ref, peer_ref, result_ref):
    span = keep_ref.shape[1]
    side, core, _ = spot()
    part = side ^ core
    for ref, at in ((keep_ref, part), (peer_ref, 1 - part)):
        result_ref[pl.ds(pl.multiple_of(at * span, 16), span), :] = ref[...].astype(F32).T.astype(BF16)


def body(
    latent,
    timestep,
    norm_gain_a,
    conv_weight_a,
    time_weight,
    norm_gain_b,
    conv_weight_b,
    norm_gain_c,
    w_query,
    w_key,
    w_value,
    w_out,
):
    rows, width, count = latent.shape
    tokens = rows * width
    share = tokens // 2
    chs = lax.axis_size("ch")
    place = lax.axis_index("row")
    core = place % 2
    image_id = place // 2
    inner = w_query.shape[0]

    def tall(weight):
        return jnp.transpose(weight, (1, 2, 0, 3)).reshape(9 * count, C)

    def halved(weight):
        depth = weight.shape[1] // 2
        return lax.dynamic_slice_in_dim(weight, core * depth, depth, axis=1)

    step_value = jnp.sum(jnp.where(jnp.arange(timestep.shape[0]) == image_id, timestep, 0)).astype(F32)
    half = TDIM // 2
    freqs = jnp.exp(-math.log(10000.0) * jnp.arange(half, dtype=F32) / half)
    angles = step_value * freqs
    sinus = jnp.concatenate([jnp.cos(angles), jnp.sin(angles)])[None, :].astype(BF16)
    field = ((2, count, share), F32)
    active = ((2, count, share), BF16)
    quarter = ((count, share), F32)
    note = ((2 * count + 16, 128), BF16)
    whole = pltpu.VMEM((C, share), BF16)

    gains = [gain.reshape(1, count) for gain in (norm_gain_a, norm_gain_b, norm_gain_c)]
    turned, keep, send, sums = call(
        enter_kernel, [((count, tokens), F32), quarter, quarter, ((count, 128), F32)], [VM] * 4
    )(latent.reshape(tokens, count), *gains)
    (active_a,) = call(first_kernel, [active], [VM] * 3)(turned, sums, swapped(sums))

    own_a, own_b = tall(conv_weight_a), tall(conv_weight_b)
    spread = jnp.broadcast_to(active_a[:, None], (2, chs // 2, count, share)).reshape(chs, count, share)
    full = lax.all_to_all(spread, "ch", 0, 0, tiled=True)
    got_a = from_beside(halved(after(own_a, spread)))
    vector, mail = call(mail_kernel, [((count, 128), F32), ((count, share + 128), F32)], [VM] * 4)(
        time_weight.T, sinus, sums, after(send, spread)
    )
    mail = crossed(mail)
    other_a = swapped(got_a)
    qkv = jnp.concatenate([w_query, w_key, w_value], axis=0)
    late_b, late, late_out, _ = lax.optimization_barrier((own_b, qkv, w_out, got_a))
    late_out = jnp.pad(halved(late_out), ((0, 0), (0, (C - w_out.shape[1]) // 2)))
    got_b = from_beside(jnp.concatenate([halved(late_b), halved(late), late_out], axis=0))

    def conv(full, own, got, other, base, near, far):
        return call(
            functools.partial(conv_kernel, near=near, far=far), [field, note], [VM] * 6, [whole]
        )(own, got, other, full, base, mail)

    def finish(part, note, act, lane_of, outs):
        return call(
            functools.partial(finish_kernel, act=act, lane_of=lane_of), outs, [VM] * 4
        )(part, image_collect(note), vector, mail)

    part_a, note_a = conv(full, own_a, got_a, other_a, vector, slice(0, 1), slice(share, share + 1))
    (active_b,) = finish(part_a, note_a, True, 1, [active])
    spread_b = column_copies(active_b)
    other_b = swapped(after(got_b, spread_b))
    part_b, note_b = conv(
        column_collect(spread_b), own_b, got_b, other_b, keep, slice(0, share), slice(0, share)
    )
    normed, hidden_b = finish(part_b, note_b, False, 2, [active, field])

    features = column_collect(column_copies(normed))

    def project(weights, at):
        return call(
            functools.partial(project_kernel, at=at),
            [((2, len(weights) * inner, share), BF16)],
            [VM] * (len(weights) + 3),
            [whole, pltpu.VMEM((len(weights) * inner, C), BF16)],
        )(*weights, got_b, other_b, features)[0]

    pairs = image_collect(project([w_key, w_value], 9 * count + inner))
    query = project([w_query], 9 * count)
    (heads_out,) = call(attend_kernel, [((2, inner, share), BF16)], [VM] * 2)(query, pairs)
    kept, sent = call(
        functools.partial(leave_kernel, at=9 * count + 3 * inner),
        [((count, share), BF16)] * 2,
        [VM] * 5,
        [pltpu.VMEM((w_out.shape[1], share), BF16)],
    )(w_out, got_b, other_b, column_collect(column_copies(heads_out)), hidden_b)
    (result,) = call(last_kernel, [((tokens, count), BF16)], [VM] * 2)(kept, crossed(sent))
    return result.reshape(rows, width, count)


def solution(mesh):
    return jax.shard_map(
        body,
        mesh=mesh,
        in_specs=(
            P("row", None, "ch"),
            P(),
            P("ch"),
            P("ch", None, None, None),
            P(None, "ch"),
            P("ch"),
            P("ch", None, None, None),
            P("ch"),
            P("ch", None),
            P("ch", None),
            P("ch", None),
            P("ch", None),
        ),
        out_specs=P("row", None, "ch"),
        check_vma=False,
    )
```

```python
import functools
import math

import jax
import jax.numpy as jnp
from jax import lax
from jax.experimental import pallas as pl
from jax.experimental.pallas import tpu as pltpu
from jax.sharding import PartitionSpec as P


C = 1280
GROUPS = 32
HEAD_DIM = 64
TDIM = 320
H = 32
W = 32
WIDE = C // GROUPS
MEMBERS = float(H * W * WIDE)
EPS = 1e-06
F32 = jnp.float32
BF16 = jnp.bfloat16

VM = pl.BlockSpec(memory_space=pltpu.VMEM)
FAR = pl.BlockSpec(memory_space=pltpu.HBM)


def call(kernel, outs, specs, scratch=()):
    return pl.pallas_call(
        kernel,
        out_shape=[jax.ShapeDtypeStruct(s, d) for s, d in outs],
        in_specs=specs,
        out_specs=[VM] * len(outs),
        scratch_shapes=list(scratch),
        compiler_params=pltpu.CompilerParams(vmem_limit_bytes=20 * 2**20),
    )


def device(ch, row):
    return ch * lax.axis_size("row") + row


def core_pairs():
    rows, chs = lax.axis_size("row"), lax.axis_size("ch")
    return [(device(k, r), device(k, r ^ 1)) for k in range(chs) for r in range(rows)]


def swapped(value):
    return lax.ppermute(value, ("ch", "row"), core_pairs())


def crossed(value):
    chs = lax.axis_size("ch")
    return lax.ppermute(value, "ch", [(k, (k + chs // 2) % chs) for k in range(chs)])


def from_beside(value):
    rows, chs = lax.axis_size("row"), lax.axis_size("ch")
    wide = 2 if rows % 4 == 0 else 1
    pairs = []
    for k in range(chs):
        for r in range(rows):
            core, high, rest = r % 2, r // 2 % wide, r // (2 * wide)
            x = (2 * high + k // (chs // 2) + (1 if core == 0 else -1)) % (2 * wide)
            source = device(x % 2 * (chs // 2) + k % (chs // 2), (rest * wide + x // 2) * 2 + core)
            pairs.append((source, device(k, r)))
    return lax.ppermute(value, ("ch", "row"), pairs)


def spot():
    side = lax.axis_index("ch") // (lax.axis_size("ch") // 2)
    core = lax.axis_index("row") % 2
    return side, core, 2 * core + (side ^ core)


def after(value, first):
    return lax.optimization_barrier((value, first))[0]


def copies(block, count):
    return jnp.broadcast_to(block[None], (count, *block.shape))


def column_copies(block):
    return copies(block, lax.axis_size("ch") // 2)


def column_collect(spread):
    half = lax.axis_size("ch") // 2
    groups = [list(range(half)), list(range(half, 2 * half))]
    return lax.all_to_all(spread, "ch", 0, 0, tiled=True, axis_index_groups=groups)


def image_collect(block):
    rows, half = lax.axis_size("row"), lax.axis_size("ch") // 2
    groups = [
        [device(k, r), device(k + half, r), device(k + half, r + 1), device(k, r + 1)]
        for r in range(0, rows, 2)
        for k in range(half)
    ]
    return lax.all_to_all(copies(block, 4), ("ch", "row"), 0, 0, tiled=True, axis_index_groups=groups)


def lanes(shape):
    return lax.broadcasted_iota(jnp.int32, shape, 1)


def silu(u):
    return u / (1.0 + jnp.exp(-u))


def scaled(value, total, squares, gain):
    mean = total / MEMBERS
    spread = squares / MEMBERS - mean * mean
    return (value - mean) * (lax.rsqrt(spread + EPS) * gain)


def by_group(per_channel):
    return [
        jnp.sum(per_channel[first : first + WIDE], axis=0, keepdims=True)
        for first in range(0, per_channel.shape[0], WIDE)
    ]


def enter_kernel(latent_ref, turned_ref, keep_ref, send_ref, sums_ref):
    side, core, _ = spot()
    value = latent_ref[...].astype(F32).T
    turned_ref[...] = value
    half = value.shape[1] // 2
    first = side == core
    keep_ref[...] = jnp.where(first, value[:, :half], value[:, half:])
    send_ref[...] = jnp.where(first, value[:, half:], value[:, :half])
    lane = lanes(sums_ref.shape)
    total = jnp.sum(value, axis=1, keepdims=True)
    squares = jnp.sum(value * value, axis=1, keepdims=True)
    sums_ref[...] = jnp.where(lane == 0, total, jnp.where(lane == 1, squares, 0.0))


def upright(rows):
    return jnp.concatenate(rows + [jnp.zeros((8 - len(rows), rows[0].shape[1]), F32)], axis=0).T


def half_kernel(weight_ref, out_ref, sem):
    _, core, _ = spot()
    depth = out_ref.shape[1]
    copy = pltpu.make_async_copy(weight_ref.at[:, pl.ds(pl.multiple_of(core * depth, 128), depth)], out_ref, sem)
    copy.start()
    copy.wait()


def first_kernel(turned_ref, own_ref, peer_ref, gain_ref, active_ref):
    _, core, _ = spot()
    sums = own_ref[...] + peer_ref[...]
    totals, squares = by_group(sums[:, 0:1]), by_group(sums[:, 1:2])
    gain = upright([gain_ref[...]])[:, 0:1]
    pieces = []
    for group in range(len(totals)):
        rows = slice(group * WIDE, (group + 1) * WIDE)
        pieces.append(scaled(turned_ref[rows], totals[group], squares[group], gain[rows]))
    value = silu(jnp.concatenate(pieces, axis=0)).astype(BF16)
    half = value.shape[1] // 2
    active_ref[core] = value[:, :half]
    active_ref[1 - core] = value[:, half:]


def mail_kernel(weight_ref, sinus_ref, gain_b_ref, gain_c_ref, send_ref, vector_ref, mail_ref):
    product = weight_ref[...].astype(F32) * sinus_ref[...].astype(F32)
    time_add = silu(jnp.sum(product, axis=1, keepdims=True))
    lane = lanes(vector_ref.shape)
    gains = upright([gain_b_ref[...], gain_c_ref[...]])
    vector = jnp.where(lane == 0, time_add, 0.0)
    for kind in range(2):
        vector = jnp.where(lane == 1 + kind, gains[:, kind : kind + 1], vector)
    vector_ref[...] = vector
    share = send_ref.shape[1]
    mail_ref[:, :share] = send_ref[...]
    mail_ref[:, share:] = vector


def gather_into(full_ref, whole_ref):
    if len(full_ref.shape) == 3:
        whole_ref[...] = full_ref[...].reshape(whole_ref.shape)
        return
    peers, _, count, _ = full_ref.shape
    for side in range(2):
        for peer in range(peers):
            at = (side * peers + peer) * count
            whole_ref[at : at + count] = full_ref[peer, side]


def both(own, gots, whole_ref):
    mine = jnp.dot(own, whole_ref[...], preferred_element_type=F32)
    if len(gots) == 1:
        return mine, jnp.dot(gots[0], whole_ref[...], preferred_element_type=F32)
    _, core, _ = spot()
    depth = gots[0].shape[1]
    near = whole_ref[pl.ds(pl.multiple_of(core * depth, 128), depth), :]
    far = whole_ref[pl.ds(pl.multiple_of((1 - core) * depth, 128), depth), :]
    theirs = jnp.dot(gots[0], near, preferred_element_type=F32)
    return mine, theirs + jnp.dot(gots[1], far, preferred_element_type=F32)


def conv_kernel(own_ref, *refs, near, far):
    *got_refs, full_ref, base_ref, far_ref, part_ref, note_ref, whole_ref = refs
    _, count, tokens = part_ref.shape
    side, _, quarter = spot()
    token = lanes((count, tokens))
    column = token % W
    lane = lanes((count, 128))
    begin = jnp.where(quarter > 0, W, 0)
    end = jnp.where(quarter < 3, tokens - W, tokens)
    gather_into(full_ref, whole_ref)
    taps = both(own_ref[...], [ref[...] for ref in got_refs], whole_ref)
    bases = base_ref[:, near], far_ref[:, far]
    extra = jnp.zeros((16, 128), F32)
    extra_lane = lanes((16, 128))
    for which in range(2):
        here = side if which == 0 else 1 - side
        combined = []
        for dy in range(3):
            left, middle, right = (
                taps[which][(3 * dy + dx) * count : (3 * dy + dx + 1) * count] for dx in range(3)
            )
            combined.append(
                middle
                + jnp.where(column == 0, 0.0, pltpu.roll(left, 1, 1))
                + jnp.where(column == W - 1, 0.0, pltpu.roll(right, tokens - 1, 1))
            )
        above, middle, below = combined
        part = (
            bases[which]
            + middle
            + jnp.where(token < W, 0.0, pltpu.roll(above, W, 1))
            + jnp.where(token >= tokens - W, 0.0, pltpu.roll(below, tokens - W, 1))
        )
        part_ref[here] = part
        kept = jnp.where(jnp.logical_and(token >= begin, token < end), part, 0.0)
        totals = by_group(jnp.sum(kept, axis=1, keepdims=True))
        squares = by_group(jnp.sum(kept * kept, axis=1, keepdims=True))
        bottom = pltpu.roll(part[:, tokens - 128 :], 2 * W, 1)
        up = pltpu.roll(below[:, :128], 2 * W, 1)
        note = jnp.where(lane < W, part[:, :128], jnp.where(lane < 2 * W, bottom, jnp.where(lane < 3 * W, up, above[:, tokens - 128 :])))
        note_ref[pl.ds(pl.multiple_of(here * count, 16), count), :] = note.astype(BF16)
        for group in range(len(totals)):
            for kind, value in enumerate((totals[group], squares[group])):
                for piece in range(3):
                    rounded = value.astype(BF16).astype(F32)
                    index = (here * len(totals) + group) * 6 + kind * 3 + piece
                    extra = jnp.where(extra_lane == index, rounded, extra)
                    value = value - rounded
    note_ref[2 * count :, :] = extra.astype(BF16)


def finish_kernel(part_ref, notes_ref, vector_ref, mail_ref, *outs, act, lane_of):
    _, count, tokens = part_ref.shape
    mine, _, quarter = spot()
    lane = lanes((count, 128))
    sums = notes_ref[0, 2 * count :].astype(F32)
    for place in range(1, 4):
        sums = sums + notes_ref[place, 2 * count :].astype(F32)
    before = jnp.maximum(quarter - 1, 0)
    after = jnp.minimum(quarter + 1, 3)
    for side in range(2):
        rows = slice(side * count, (side + 1) * count)
        notes = [notes_ref[place, rows].astype(F32) for place in range(4)]
        total = jnp.zeros((count, 1), F32)
        squares = jnp.zeros((count, 1), F32)
        for low in range(3):
            one, two = notes[low], notes[low + 1]
            edges = jnp.where(
                lane < W,
                two + pltpu.roll(one, W, 1),
                jnp.where(lane < 2 * W, one + pltpu.roll(two, 128 - W, 1), 0.0),
            )
            total = total + jnp.sum(edges, axis=1, keepdims=True)
            squares = squares + jnp.sum(edges * edges, axis=1, keepdims=True)
        top = pltpu.roll(notes_ref[before, rows].astype(F32), W, 1)
        low = pltpu.roll(notes_ref[after, rows].astype(F32), W, 1)
        part = part_ref[side]
        value = jnp.concatenate(
            [
                part[:, :128] + jnp.where(lane < jnp.where(quarter > 0, W, 0), top, 0.0),
                part[:, tokens - 128 :] + jnp.where(lane >= jnp.where(quarter < 3, 128 - W, 128), low, 0.0),
            ],
            axis=1,
        )
        totals, squared = by_group(total), by_group(squares)
        at = tokens + lane_of
        gain = jnp.where(side == mine, vector_ref[:, lane_of : lane_of + 1], mail_ref[:, at : at + 1])
        pieces = []
        for group in range(len(totals)):
            first = (side * len(totals) + group) * 6
            whole = totals[group] + jnp.sum(sums[0:1, first : first + 3], axis=1, keepdims=True)
            whole_squares = squared[group] + jnp.sum(sums[0:1, first + 3 : first + 6], axis=1, keepdims=True)
            span = slice(group * WIDE, (group + 1) * WIDE)
            pieces.append(scaled(value[span], whole, whole_squares, gain[span]))
        result = jnp.concatenate(pieces, axis=0)
        if act:
            outs[0][side] = silu(result).astype(BF16)
        else:
            outs[0][side] = result.astype(BF16)
            outs[1][side] = value


def project_kernel(*refs, at):
    *own_refs, got_ref, full_ref, out_ref, whole_ref, stack_ref = refs
    inner = own_refs[0].shape[0]
    side, _, _ = spot()
    for index, ref in enumerate(own_refs):
        stack_ref[index * inner : (index + 1) * inner] = ref[...]
    gather_into(full_ref, whole_ref)
    rows = slice(at, at + len(own_refs) * inner)
    mixed = both(stack_ref[...], [got_ref[rows]], whole_ref)
    for which in range(2):
        out_ref[side if which == 0 else 1 - side] = mixed[which].astype(BF16)


def attend_kernel(q_ref, pairs_ref, out_ref):
    inner = q_ref.shape[1]
    for head in range(2):
        keys = jnp.concatenate([pairs_ref[place, head, :inner] for place in range(4)], axis=1)
        values = jnp.concatenate([pairs_ref[place, head, inner:] for place in range(4)], axis=1)
        scores = lax.dot_general(
            keys, q_ref[head], (((0,), (0,)), ((), ())), preferred_element_type=F32
        ) * (1.0 / math.sqrt(HEAD_DIM))
        raised = jnp.exp(scores - jnp.max(scores, axis=0, keepdims=True))
        weights = (raised * (1.0 / jnp.sum(raised, axis=0, keepdims=True))).astype(BF16)
        out_ref[head] = jnp.dot(values, weights, preferred_element_type=F32).astype(BF16)


def leave_kernel(weight_ref, got_ref, full_ref, hidden_ref, keep_ref, send_ref, whole_ref, *, at):
    count, depth = weight_ref.shape
    side, _, _ = spot()
    gather_into(full_ref, whole_ref)
    mine, theirs = both(weight_ref[...], [got_ref[at : at + count, :depth]], whole_ref)
    keep_ref[...] = (hidden_ref[side] + mine).astype(BF16)
    send_ref[...] = (hidden_ref[1 - side] + theirs).astype(BF16)


def last_kernel(keep_ref, peer_ref, result_ref):
    span = keep_ref.shape[1]
    side, core, _ = spot()
    part = side ^ core
    for ref, at in ((keep_ref, part), (peer_ref, 1 - part)):
        result_ref[pl.ds(pl.multiple_of(at * span, 16), span), :] = ref[...].astype(F32).T.astype(BF16)


def body(
    latent,
    timestep,
    norm_gain_a,
    conv_weight_a,
    time_weight,
    norm_gain_b,
    conv_weight_b,
    norm_gain_c,
    w_query,
    w_key,
    w_value,
    w_out,
):
    rows, width, count = latent.shape
    tokens = rows * width
    share = tokens // 2
    chs = lax.axis_size("ch")
    place = lax.axis_index("row")
    image_id = place // 2
    inner = w_query.shape[0]

    def tall(weight):
        return jnp.transpose(weight, (1, 2, 0, 3)).reshape(9 * count, C)

    step_value = jnp.sum(jnp.where(jnp.arange(timestep.shape[0]) == image_id, timestep, 0)).astype(F32)
    half = TDIM // 2
    freqs = jnp.exp(-math.log(10000.0) * jnp.arange(half, dtype=F32) / half)
    angles = step_value * freqs
    sinus = jnp.concatenate([jnp.cos(angles), jnp.sin(angles)])[None, :].astype(BF16)
    field = ((2, count, share), F32)
    active = ((2, count, share), BF16)
    quarter = ((count, share), F32)
    note = ((2 * count + 16, 128), BF16)
    whole = pltpu.VMEM((C, share), BF16)

    gain_a, gain_b, gain_c = (gain.reshape(1, count) for gain in (norm_gain_a, norm_gain_b, norm_gain_c))
    own_a, own_b = tall(conv_weight_a), tall(conv_weight_b)
    turned, keep, send, sums = call(
        enter_kernel, [((count, tokens), F32), quarter, quarter, ((count, 128), F32)], [VM]
    )(latent.reshape(tokens, count))
    peer = swapped(sums)
    (half_a,) = call(half_kernel, [((9 * count, C // 2), BF16)], [FAR], [pltpu.SemaphoreType.DMA])(
        after(own_a, sums)
    )
    got_a = from_beside(half_a)
    (active_a,) = call(first_kernel, [active], [VM] * 4)(turned, sums, peer, gain_a)

    spread = jnp.broadcast_to(active_a[:, None], (2, chs // 2, count, share)).reshape(chs, count, share)
    full = lax.all_to_all(spread, "ch", 0, 0, tiled=True)
    vector, mail = call(mail_kernel, [((count, 128), F32), ((count, share + 128), F32)], [VM] * 5)(
        time_weight.T, sinus, gain_b, gain_c, after(send, spread)
    )
    mail = crossed(mail)
    other_a = swapped(after(got_a, spread))

    def conv(full, own, gots, base, near, far):
        return call(
            functools.partial(conv_kernel, near=near, far=far), [field, note], [VM] * (4 + len(gots)), [whole]
        )(own, *gots, full, base, mail)

    def finish(part, note, act, lane_of, outs):
        return call(
            functools.partial(finish_kernel, act=act, lane_of=lane_of), outs, [VM] * 4
        )(part, image_collect(note), vector, mail)

    part_a, note_a = conv(full, own_a, [got_a, other_a], vector, slice(0, 1), slice(share, share + 1))
    (active_b,) = finish(part_a, note_a, True, 1, [active])
    spread_b = column_copies(active_b)
    full_b = column_collect(spread_b)
    got_b = from_beside(after(own_b, spread_b))
    part_b, note_b = conv(full_b, own_b, [got_b], keep, slice(0, share), slice(0, share))
    normed, hidden_b = finish(part_b, note_b, False, 2, [active, field])

    spread_c = column_copies(normed)
    features = column_collect(spread_c)
    late = [after(weight, note_b) for weight in (w_query, w_key, w_value)]
    late.append(jnp.pad(after(w_out, note_b), ((0, 0), (0, C - w_out.shape[1]))))
    got_c = from_beside(after(jnp.concatenate(late, axis=0), spread_c))

    def project(weights, at):
        return call(
            functools.partial(project_kernel, at=at),
            [((2, len(weights) * inner, share), BF16)],
            [VM] * (len(weights) + 2),
            [whole, pltpu.VMEM((len(weights) * inner, C), BF16)],
        )(*weights, got_c, features)[0]

    pairs = image_collect(project([w_key, w_value], inner))
    query = project([w_query], 0)
    (heads_out,) = call(attend_kernel, [((2, inner, share), BF16)], [VM] * 2)(query, pairs)
    kept, sent = call(
        functools.partial(leave_kernel, at=3 * inner),
        [((count, share), BF16)] * 2,
        [VM] * 4,
        [pltpu.VMEM((w_out.shape[1], share), BF16)],
    )(w_out, got_c, column_collect(column_copies(heads_out)), hidden_b)
    (result,) = call(last_kernel, [((tokens, count), BF16)], [VM] * 2)(kept, crossed(sent))
    return result.reshape(rows, width, count)


def solution(mesh):
    return jax.shard_map(
        body,
        mesh=mesh,
        in_specs=(
            P("row", None, "ch"),
            P(),
            P("ch"),
            P("ch", None, None, None),
            P(None, "ch"),
            P("ch"),
            P("ch", None, None, None),
            P("ch"),
            P("ch", None),
            P("ch", None),
            P("ch", None),
            P("ch", None),
        ),
        out_specs=P("row", None, "ch"),
        check_vma=False,
    )
```

```python
import functools
import math

import jax
import jax.numpy as jnp
from jax import lax
from jax.experimental import pallas as pl
from jax.experimental.pallas import tpu as pltpu
from jax.sharding import PartitionSpec as P


C = 1280
GROUPS = 32
HEAD_DIM = 64
TDIM = 320
H = 32
W = 32
WIDE = C // GROUPS
MEMBERS = float(H * W * WIDE)
EPS = 1e-06
F32 = jnp.float32
BF16 = jnp.bfloat16

VM = pl.BlockSpec(memory_space=pltpu.VMEM)
FAR = pl.BlockSpec(memory_space=pltpu.HBM)


def call(kernel, outs, specs, scratch=()):
    return pl.pallas_call(
        kernel,
        out_shape=[jax.ShapeDtypeStruct(s, d) for s, d in outs],
        in_specs=specs,
        out_specs=[VM] * len(outs),
        scratch_shapes=list(scratch),
        compiler_params=pltpu.CompilerParams(vmem_limit_bytes=20 * 2**20),
    )


def device(ch, row):
    return ch * lax.axis_size("row") + row


def core_pairs():
    rows, chs = lax.axis_size("row"), lax.axis_size("ch")
    return [(device(k, r), device(k, r ^ 1)) for k in range(chs) for r in range(rows)]


def swapped(value):
    return lax.ppermute(value, ("ch", "row"), core_pairs())


def crossed(value):
    chs = lax.axis_size("ch")
    return lax.ppermute(value, "ch", [(k, (k + chs // 2) % chs) for k in range(chs)])


def from_beside(value):
    rows, chs = lax.axis_size("row"), lax.axis_size("ch")
    wide = 2 if rows % 4 == 0 else 1
    pairs = []
    for k in range(chs):
        for r in range(rows):
            core, high, rest = r % 2, r // 2 % wide, r // (2 * wide)
            side = k // (chs // 2)
            x = (2 * high + side + (1 if side else -1)) % (2 * wide)
            source = device(x % 2 * (chs // 2) + k % (chs // 2), (rest * wide + x // 2) * 2 + core)
            pairs.append((source, device(k, r)))
    return lax.ppermute(value, ("ch", "row"), pairs)


def spot():
    side = lax.axis_index("ch") // (lax.axis_size("ch") // 2)
    core = lax.axis_index("row") % 2
    return side, core, 2 * core + (side ^ core)


def after(value, first):
    return lax.optimization_barrier((value, first))[0]


def column_collect(spread):
    half = lax.axis_size("ch") // 2
    groups = [list(range(half)), list(range(half, 2 * half))]
    return lax.all_to_all(spread, "ch", 0, 0, tiled=True, axis_index_groups=groups)


def image_collect(spread):
    rows, half = lax.axis_size("row"), lax.axis_size("ch") // 2
    groups = [
        [device(k, r), device(k + half, r), device(k + half, r + 1), device(k, r + 1)]
        for r in range(0, rows, 2)
        for k in range(half)
    ]
    return lax.all_to_all(spread, ("ch", "row"), 0, 0, tiled=True, axis_index_groups=groups)


def lanes(shape):
    return lax.broadcasted_iota(jnp.int32, shape, 1)


def silu(u):
    return u / (1.0 + jnp.exp(-u))


def scaled(value, total, squares, gain):
    mean = total / MEMBERS
    spread = squares / MEMBERS - mean * mean
    return (value - mean) * (lax.rsqrt(spread + EPS) * gain)


def by_group(per_channel):
    return [
        jnp.sum(per_channel[first : first + WIDE], axis=0, keepdims=True)
        for first in range(0, per_channel.shape[0], WIDE)
    ]


def enter_kernel(latent_ref, weight_ref, turned_ref, sums_ref, half_ref, sem):
    _, core, _ = spot()
    depth = half_ref.shape[1]
    columns = pl.ds(pl.multiple_of(core * depth, 128), depth)
    copy = pltpu.make_async_copy(weight_ref.at[:, columns], half_ref, sem)
    copy.start()
    value = latent_ref[...].astype(F32).T
    turned_ref[...] = value
    lane = lanes(sums_ref.shape)
    total = jnp.sum(value, axis=1, keepdims=True)
    squares = jnp.sum(value * value, axis=1, keepdims=True)
    sums_ref[...] = jnp.where(lane == 0, total, jnp.where(lane == 1, squares, 0.0))
    copy.wait()


def upright(rows):
    return jnp.concatenate(rows + [jnp.zeros((8 - len(rows), rows[0].shape[1]), F32)], axis=0).T


def first_kernel(turned_ref, own_ref, peer_ref, gain_ref, active_ref):
    _, core, _ = spot()
    sums = own_ref[...] + peer_ref[...]
    totals, squares = by_group(sums[:, 0:1]), by_group(sums[:, 1:2])
    gain = upright([gain_ref[...]])[:, 0:1]
    pieces = []
    for group in range(len(totals)):
        rows = slice(group * WIDE, (group + 1) * WIDE)
        pieces.append(scaled(turned_ref[rows], totals[group], squares[group], gain[rows]))
    value = silu(jnp.concatenate(pieces, axis=0)).astype(BF16)
    half = value.shape[1] // 2
    each = active_ref.shape[0] // 2
    for copy in range(each):
        active_ref[core * each + copy] = value[:, :half]
        active_ref[(1 - core) * each + copy] = value[:, half:]


def time_of(weight_ref, sinus_ref):
    product = weight_ref[...].astype(F32) * sinus_ref[...].astype(F32)
    return silu(jnp.sum(product, axis=1, keepdims=True))


def turned_share(latent_ref, part, share):
    rows = pl.ds(pl.multiple_of(part * share, 16), share)
    return latent_ref[rows, :].astype(F32).T


def mail_kernel(weight_ref, sinus_ref, gain_b_ref, gain_c_ref, latent_ref, mail_ref):
    side, core, _ = spot()
    share = latent_ref.shape[0] // 2
    lane = lanes((mail_ref.shape[0], 128))
    gains = upright([gain_b_ref[...], gain_c_ref[...]])
    vector = jnp.where(lane == 0, time_of(weight_ref, sinus_ref), 0.0)
    for kind in range(2):
        vector = jnp.where(lane == 1 + kind, gains[:, kind : kind + 1], vector)
    mail_ref[:, :share] = turned_share(latent_ref, 1 - (side ^ core), share)
    mail_ref[:, share:] = vector


def gather_into(full_ref, whole_ref):
    if len(full_ref.shape) == 3:
        whole_ref[...] = full_ref[...].reshape(whole_ref.shape)
        return
    peers, _, count, _ = full_ref.shape
    for side in range(2):
        for peer in range(peers):
            at = (side * peers + peer) * count
            whole_ref[at : at + count] = full_ref[peer, side]


def both(own, gots, whole_ref):
    mine = jnp.dot(own, whole_ref[...], preferred_element_type=F32)
    depth = gots[0].shape[1]
    if depth == own.shape[1]:
        pieces = [jnp.dot(got, whole_ref[...], preferred_element_type=F32) for got in gots]
        return mine, jnp.concatenate(pieces, axis=0)
    _, core, _ = spot()
    near = whole_ref[pl.ds(pl.multiple_of(core * depth, 128), depth), :]
    far = whole_ref[pl.ds(pl.multiple_of((1 - core) * depth, 128), depth), :]
    theirs = jnp.dot(gots[0], near, preferred_element_type=F32)
    return mine, theirs + jnp.dot(gots[1], far, preferred_element_type=F32)


def conv_kernel(own_ref, *refs, gots):
    got_refs, refs = refs[:gots], refs[gots:]
    full_ref, mail_ref, *base_refs, part_ref, note_ref, whole_ref = refs
    _, count, tokens = part_ref.shape
    side, core, quarter = spot()
    token = lanes((count, tokens))
    column = token % W
    lane = lanes((count, 128))
    begin = jnp.where(quarter > 0, W, 0)
    end = jnp.where(quarter < 3, tokens - W, tokens)
    gather_into(full_ref, whole_ref)
    taps = both(own_ref[...], [ref[...] for ref in got_refs], whole_ref)
    if len(base_refs) == 2:
        bases = time_of(*base_refs), mail_ref[:, tokens : tokens + 1]
    else:
        bases = turned_share(base_refs[0], side ^ core, tokens), mail_ref[:, :tokens]
    extra = jnp.zeros((16, 128), F32)
    extra_lane = lanes((16, 128))
    for which in range(2):
        here = side if which == 0 else 1 - side
        combined = []
        for dy in range(3):
            left, middle, right = (
                taps[which][(3 * dy + dx) * count : (3 * dy + dx + 1) * count] for dx in range(3)
            )
            combined.append(
                middle
                + jnp.where(column == 0, 0.0, pltpu.roll(left, 1, 1))
                + jnp.where(column == W - 1, 0.0, pltpu.roll(right, tokens - 1, 1))
            )
        above, middle, below = combined
        part = (
            bases[which]
            + middle
            + jnp.where(token < W, 0.0, pltpu.roll(above, W, 1))
            + jnp.where(token >= tokens - W, 0.0, pltpu.roll(below, tokens - W, 1))
        )
        part_ref[here] = part
        kept = jnp.where(jnp.logical_and(token >= begin, token < end), part, 0.0)
        totals = by_group(jnp.sum(kept, axis=1, keepdims=True))
        squares = by_group(jnp.sum(kept * kept, axis=1, keepdims=True))
        bottom = pltpu.roll(part[:, tokens - 128 :], 2 * W, 1)
        up = pltpu.roll(below[:, :128], 2 * W, 1)
        note = jnp.where(lane < W, part[:, :128], jnp.where(lane < 2 * W, bottom, jnp.where(lane < 3 * W, up, above[:, tokens - 128 :])))
        for copy in range(note_ref.shape[0]):
            note_ref[copy, pl.ds(pl.multiple_of(here * count, 16), count), :] = note.astype(BF16)
        for group in range(len(totals)):
            for kind, value in enumerate((totals[group], squares[group])):
                for piece in range(3):
                    rounded = value.astype(BF16).astype(F32)
                    index = (here * len(totals) + group) * 6 + kind * 3 + piece
                    extra = jnp.where(extra_lane == index, rounded, extra)
                    value = value - rounded
    for copy in range(note_ref.shape[0]):
        note_ref[copy, 2 * count :, :] = extra.astype(BF16)


def finish_kernel(part_ref, notes_ref, gain_ref, mail_ref, *outs, act, lane_of):
    _, count, tokens = part_ref.shape
    mine, _, quarter = spot()
    own_gain = upright([gain_ref[...]])[:, 0:1]
    lane = lanes((count, 128))
    sums = notes_ref[0, 2 * count :].astype(F32)
    for place in range(1, 4):
        sums = sums + notes_ref[place, 2 * count :].astype(F32)
    before = jnp.maximum(quarter - 1, 0)
    after = jnp.minimum(quarter + 1, 3)
    for side in range(2):
        rows = slice(side * count, (side + 1) * count)
        notes = [notes_ref[place, rows].astype(F32) for place in range(4)]
        total = jnp.zeros((count, 1), F32)
        squares = jnp.zeros((count, 1), F32)
        for low in range(3):
            one, two = notes[low], notes[low + 1]
            edges = jnp.where(
                lane < W,
                two + pltpu.roll(one, W, 1),
                jnp.where(lane < 2 * W, one + pltpu.roll(two, 128 - W, 1), 0.0),
            )
            total = total + jnp.sum(edges, axis=1, keepdims=True)
            squares = squares + jnp.sum(edges * edges, axis=1, keepdims=True)
        top = pltpu.roll(notes_ref[before, rows].astype(F32), W, 1)
        low = pltpu.roll(notes_ref[after, rows].astype(F32), W, 1)
        part = part_ref[side]
        value = jnp.concatenate(
            [
                part[:, :128] + jnp.where(lane < jnp.where(quarter > 0, W, 0), top, 0.0),
                part[:, tokens - 128 :] + jnp.where(lane >= jnp.where(quarter < 3, 128 - W, 128), low, 0.0),
            ],
            axis=1,
        )
        totals, squared = by_group(total), by_group(squares)
        at = tokens + lane_of
        gain = jnp.where(side == mine, own_gain, mail_ref[:, at : at + 1])
        pieces = []
        for group in range(len(totals)):
            first = (side * len(totals) + group) * 6
            whole = totals[group] + jnp.sum(sums[0:1, first : first + 3], axis=1, keepdims=True)
            whole_squares = squared[group] + jnp.sum(sums[0:1, first + 3 : first + 6], axis=1, keepdims=True)
            span = slice(group * WIDE, (group + 1) * WIDE)
            pieces.append(scaled(value[span], whole, whole_squares, gain[span]))
        result = jnp.concatenate(pieces, axis=0)
        result = (silu(result) if act else result).astype(BF16)
        for copy in range(outs[0].shape[0]):
            outs[0][copy, side] = result
        if not act:
            outs[1][side] = value


def project_kernel(query_ref, key_ref, value_ref, got_ref, full_ref, q_ref, kv_ref, whole_ref, stack_ref):
    inner = query_ref.shape[0]
    side, _, _ = spot()
    for index, ref in enumerate((query_ref, key_ref, value_ref)):
        stack_ref[index * inner : (index + 1) * inner] = ref[...]
    gather_into(full_ref, whole_ref)
    mixed = both(stack_ref[...], [got_ref[: 3 * inner]], whole_ref)
    for which in range(2):
        here = side if which == 0 else 1 - side
        q_ref[here] = mixed[which][:inner].astype(BF16)
        for copy in range(kv_ref.shape[0]):
            kv_ref[copy, here] = mixed[which][inner:].astype(BF16)


def attend_kernel(q_ref, pairs_ref, out_ref):
    inner = q_ref.shape[1]
    for head in range(2):
        keys = jnp.concatenate([pairs_ref[place, head, :inner] for place in range(4)], axis=1)
        values = jnp.concatenate([pairs_ref[place, head, inner:] for place in range(4)], axis=1)
        scores = lax.dot_general(
            keys, q_ref[head], (((0,), (0,)), ((), ())), preferred_element_type=F32
        ) * (1.0 / math.sqrt(HEAD_DIM))
        raised = jnp.exp(scores - jnp.max(scores, axis=0, keepdims=True))
        weights = (raised * (1.0 / jnp.sum(raised, axis=0, keepdims=True))).astype(BF16)
        mixed = jnp.dot(values, weights, preferred_element_type=F32).astype(BF16)
        for copy in range(out_ref.shape[0]):
            out_ref[copy, head] = mixed


def leave_kernel(weight_ref, got_ref, full_ref, hidden_ref, keep_ref, send_ref, whole_ref, *, at):
    count, depth = weight_ref.shape
    side, _, _ = spot()
    gather_into(full_ref, whole_ref)
    mine, theirs = both(weight_ref[...], [got_ref[at : at + count, :depth]], whole_ref)
    keep_ref[...] = (hidden_ref[side] + mine).astype(BF16)
    send_ref[...] = (hidden_ref[1 - side] + theirs).astype(BF16)


def last_kernel(keep_ref, peer_ref, result_ref):
    span = keep_ref.shape[1]
    side, core, _ = spot()
    part = side ^ core
    for ref, at in ((keep_ref, part), (peer_ref, 1 - part)):
        result_ref[pl.ds(pl.multiple_of(at * span, 16), span), :] = ref[...].astype(F32).T.astype(BF16)


def body(
    latent,
    timestep,
    norm_gain_a,
    conv_weight_a,
    time_weight,
    norm_gain_b,
    conv_weight_b,
    norm_gain_c,
    w_query,
    w_key,
    w_value,
    w_out,
):
    rows, width, count = latent.shape
    tokens = rows * width
    share = tokens // 2
    chs = lax.axis_size("ch")
    place = lax.axis_index("row")
    image_id = place // 2
    inner = w_query.shape[0]

    def tall(weight):
        return jnp.transpose(weight, (1, 2, 0, 3)).reshape(9 * count, C)

    step_value = jnp.sum(jnp.where(jnp.arange(timestep.shape[0]) == image_id, timestep, 0)).astype(F32)
    half = TDIM // 2
    freqs = jnp.exp(-math.log(10000.0) * jnp.arange(half, dtype=F32) / half)
    angles = step_value * freqs
    sinus = jnp.concatenate([jnp.cos(angles), jnp.sin(angles)])[None, :].astype(BF16)
    field = ((2, count, share), F32)
    half_chs = chs // 2
    active = ((half_chs, 2, count, share), BF16)
    note = ((4, 2 * count + 16, 128), BF16)
    whole = pltpu.VMEM((C, share), BF16)

    gain_a, gain_b, gain_c = (gain.reshape(1, count) for gain in (norm_gain_a, norm_gain_b, norm_gain_c))
    own_a, own_b = tall(conv_weight_a), tall(conv_weight_b)
    flat = latent.reshape(tokens, count)
    turned, sums, half_a = call(
        enter_kernel,
        [((count, tokens), F32), ((count, 128), F32), ((9 * count, C // 2), BF16)],
        [VM, FAR],
        [pltpu.SemaphoreType.DMA],
    )(flat, own_a)
    peer = swapped(sums)
    got_a = from_beside(half_a)
    (spread_a,) = call(first_kernel, [((chs, count, share), BF16)], [VM] * 4)(turned, sums, peer, gain_a)

    full = lax.all_to_all(spread_a, "ch", 0, 0, tiled=True)
    (mail,) = call(mail_kernel, [((count, share + 128), F32)], [VM] * 5)(
        time_weight.T, sinus, gain_b, gain_c, after(flat, spread_a)
    )
    mail = crossed(mail)
    cut = 6 * count
    late_b = after(own_b, spread_a)
    low_b = crossed(late_b[cut:])
    high_b = from_beside(late_b[:cut])
    late = [w_query, w_key, w_value, jnp.pad(w_out, ((0, 0), (0, C - w_out.shape[1])))]
    got_c = from_beside(after(jnp.concatenate(late, axis=0), spread_a))
    other_a = swapped(after(got_a, spread_a))

    def conv(full, own, gots, *bases):
        return call(
            functools.partial(conv_kernel, gots=len(gots)),
            [field, note],
            [VM] * (3 + len(gots) + len(bases)),
            [whole],
        )(own, *gots, full, mail, *bases)

    def finish(part, notes, gain, act, lane_of, outs):
        return call(
            functools.partial(finish_kernel, act=act, lane_of=lane_of), outs, [VM] * 4
        )(part, notes, gain, mail)

    part_a, note_a = conv(full, own_a, [got_a, other_a], time_weight.T, sinus)
    notes_a = image_collect(note_a)
    (spread_b,) = finish(part_a, notes_a, gain_b, True, 1, [active])
    part_b, note_b = conv(column_collect(spread_b), own_b, [high_b, low_b], flat)
    notes_b = image_collect(note_b)
    spread_c, hidden_b = finish(part_b, notes_b, gain_c, False, 2, [active, field])
    features = column_collect(spread_c)

    query, key_value = call(
        project_kernel,
        [((2, inner, share), BF16), ((4, 2, 2 * inner, share), BF16)],
        [VM] * 5,
        [whole, pltpu.VMEM((3 * inner, C), BF16)],
    )(w_query, w_key, w_value, got_c, features)
    pairs = image_collect(key_value)
    (heads_out,) = call(attend_kernel, [((half_chs, 2, inner, share), BF16)], [VM] * 2)(query, pairs)
    kept, sent = call(
        functools.partial(leave_kernel, at=3 * inner),
        [((count, share), BF16)] * 2,
        [VM] * 4,
        [pltpu.VMEM((w_out.shape[1], share), BF16)],
    )(w_out, got_c, column_collect(heads_out), hidden_b)
    (result,) = call(last_kernel, [((tokens, count), BF16)], [VM] * 2)(kept, crossed(sent))
    return result.reshape(rows, width, count)


def solution(mesh):
    return jax.shard_map(
        body,
        mesh=mesh,
        in_specs=(
            P("row", None, "ch"),
            P(),
            P("ch"),
            P("ch", None, None, None),
            P(None, "ch"),
            P("ch"),
            P("ch", None, None, None),
            P("ch"),
            P("ch", None),
            P("ch", None),
            P("ch", None),
            P("ch", None),
        ),
        out_specs=P("row", None, "ch"),
        check_vma=False,
    )
```

```python
import functools
import math

import jax
import jax.numpy as jnp
from jax import lax
from jax.experimental import pallas as pl
from jax.experimental.pallas import tpu as pltpu
from jax.sharding import PartitionSpec as P


C = 1280
GROUPS = 32
HEAD_DIM = 64
TDIM = 320
H = 32
W = 32
WIDE = C // GROUPS
MEMBERS = float(H * W * WIDE)
EPS = 1e-06
F32 = jnp.float32
BF16 = jnp.bfloat16

VM = pl.BlockSpec(memory_space=pltpu.VMEM)
FAR = pl.BlockSpec(memory_space=pltpu.HBM)


def call(kernel, outs, specs, scratch=(), limit=20 * 2**20):
    return pl.pallas_call(
        kernel,
        out_shape=[jax.ShapeDtypeStruct(s, d) for s, d in outs],
        in_specs=specs,
        out_specs=[VM] * len(outs),
        scratch_shapes=list(scratch),
        compiler_params=pltpu.CompilerParams(vmem_limit_bytes=limit),
    )


def device(ch, row):
    return ch * lax.axis_size("row") + row


def core_pairs():
    rows, chs = lax.axis_size("row"), lax.axis_size("ch")
    return [(device(k, r), device(k, r ^ 1)) for k in range(chs) for r in range(rows)]


def swapped(value):
    return lax.ppermute(value, ("ch", "row"), core_pairs())


def crossed(value):
    chs = lax.axis_size("ch")
    return lax.ppermute(value, "ch", [(k, (k + chs // 2) % chs) for k in range(chs)])


def from_beside(value):
    rows, chs = lax.axis_size("row"), lax.axis_size("ch")
    wide = 2 if rows % 4 == 0 else 1
    pairs = []
    for k in range(chs):
        for r in range(rows):
            core, high, rest = r % 2, r // 2 % wide, r // (2 * wide)
            side = k // (chs // 2)
            x = (2 * high + side + (1 if side else -1)) % (2 * wide)
            source = device(x % 2 * (chs // 2) + k % (chs // 2), (rest * wide + x // 2) * 2 + core)
            pairs.append((source, device(k, r)))
    return lax.ppermute(value, ("ch", "row"), pairs)


def spot():
    side = lax.axis_index("ch") // (lax.axis_size("ch") // 2)
    core = lax.axis_index("row") % 2
    return side, core, 2 * core + (side ^ core)


def after(value, first):
    return lax.optimization_barrier((value, first))[0]


def column_collect(spread):
    half = lax.axis_size("ch") // 2
    groups = [list(range(half)), list(range(half, 2 * half))]
    return lax.all_to_all(spread, "ch", 0, 0, tiled=True, axis_index_groups=groups)


def image_collect(spread):
    rows, half = lax.axis_size("row"), lax.axis_size("ch") // 2
    groups = [
        [device(k, r), device(k + half, r), device(k + half, r + 1), device(k, r + 1)]
        for r in range(0, rows, 2)
        for k in range(half)
    ]
    return lax.all_to_all(spread, ("ch", "row"), 0, 0, tiled=True, axis_index_groups=groups)


def lanes(shape):
    return lax.broadcasted_iota(jnp.int32, shape, 1)


def silu(u):
    return u / (1.0 + jnp.exp(-u))


def scaled(value, total, squares, gain):
    mean = total / MEMBERS
    spread = squares / MEMBERS - mean * mean
    return (value - mean) * (lax.rsqrt(spread + EPS) * gain)


def by_group(per_channel):
    return [
        jnp.sum(per_channel[first : first + WIDE], axis=0, keepdims=True)
        for first in range(0, per_channel.shape[0], WIDE)
    ]


def enter_kernel(latent_ref, weight_ref, turned_ref, sums_ref, half_ref, sem):
    _, core, _ = spot()
    depth = half_ref.shape[1]
    columns = pl.ds(pl.multiple_of(core * depth, 128), depth)
    copy = pltpu.make_async_copy(weight_ref.at[:, columns], half_ref, sem)
    copy.start()
    value = latent_ref[...].astype(F32).T
    turned_ref[...] = value
    lane = lanes(sums_ref.shape)
    total = jnp.sum(value, axis=1, keepdims=True)
    squares = jnp.sum(value * value, axis=1, keepdims=True)
    sums_ref[...] = jnp.where(lane == 0, total, jnp.where(lane == 1, squares, 0.0))
    copy.wait()


def upright(rows):
    return jnp.concatenate(rows + [jnp.zeros((8 - len(rows), rows[0].shape[1]), F32)], axis=0).T


def first_kernel(turned_ref, own_ref, peer_ref, gain_ref, active_ref):
    _, core, _ = spot()
    sums = own_ref[...] + peer_ref[...]
    totals, squares = by_group(sums[:, 0:1]), by_group(sums[:, 1:2])
    gain = upright([gain_ref[...]])[:, 0:1]
    pieces = []
    for group in range(len(totals)):
        rows = slice(group * WIDE, (group + 1) * WIDE)
        pieces.append(scaled(turned_ref[rows], totals[group], squares[group], gain[rows]))
    value = silu(jnp.concatenate(pieces, axis=0)).astype(BF16)
    half = value.shape[1] // 2
    each = active_ref.shape[0] // 2
    for copy in range(each):
        active_ref[core * each + copy] = value[:, :half]
        active_ref[(1 - core) * each + copy] = value[:, half:]


def time_of(weight_ref, sinus_ref):
    product = weight_ref[...].astype(F32) * sinus_ref[...].astype(F32)
    return silu(jnp.sum(product, axis=1, keepdims=True))


def turned_share(latent_ref, part, share):
    rows = pl.ds(pl.multiple_of(part * share, 16), share)
    return latent_ref[rows, :].astype(F32).T


def mail_kernel(weight_ref, sinus_ref, gain_b_ref, gain_c_ref, latent_ref, mail_ref):
    side, core, _ = spot()
    share = latent_ref.shape[0] // 2
    lane = lanes((mail_ref.shape[0], 128))
    gains = upright([gain_b_ref[...], gain_c_ref[...]])
    vector = jnp.where(lane == 0, time_of(weight_ref, sinus_ref), 0.0)
    for kind in range(2):
        vector = jnp.where(lane == 1 + kind, gains[:, kind : kind + 1], vector)
    mail_ref[:, :share] = turned_share(latent_ref, 1 - (side ^ core), share)
    mail_ref[:, share:] = vector


def gather_into(full_ref, whole_ref):
    if len(full_ref.shape) == 3:
        whole_ref[...] = full_ref[...].reshape(whole_ref.shape)
        return
    peers, _, count, _ = full_ref.shape
    for side in range(2):
        for peer in range(peers):
            at = (side * peers + peer) * count
            whole_ref[at : at + count] = full_ref[peer, side]


def both(own, gots, whole_ref):
    mine = jnp.dot(own, whole_ref[...], preferred_element_type=F32)
    depth = gots[0].shape[1]
    if len(gots) == 1:
        return mine, jnp.dot(gots[0], whole_ref[...], preferred_element_type=F32)
    _, core, _ = spot()
    near = whole_ref[pl.ds(pl.multiple_of(core * depth, 128), depth), :]
    far = whole_ref[pl.ds(pl.multiple_of((1 - core) * depth, 128), depth), :]
    theirs = jnp.dot(gots[0], near, preferred_element_type=F32)
    return mine, theirs + jnp.dot(gots[1], far, preferred_element_type=F32)


def conv_kernel(own_ref, *refs, gots):
    got_refs, refs = refs[:gots], refs[gots:]
    full_ref, mail_ref, *base_refs, part_ref, note_ref, whole_ref = refs
    _, count, tokens = part_ref.shape
    side, core, quarter = spot()
    token = lanes((count, tokens))
    column = token % W
    lane = lanes((count, 128))
    begin = jnp.where(quarter > 0, W, 0)
    end = jnp.where(quarter < 3, tokens - W, tokens)
    gather_into(full_ref, whole_ref)
    taps = both(own_ref[...], [ref[...] for ref in got_refs], whole_ref)
    if len(base_refs) == 2:
        bases = time_of(*base_refs), mail_ref[:, tokens : tokens + 1]
    else:
        bases = turned_share(base_refs[0], side ^ core, tokens), mail_ref[:, :tokens]
    extra = jnp.zeros((16, 128), F32)
    extra_lane = lanes((16, 128))
    for which in range(2):
        here = side if which == 0 else 1 - side
        combined = []
        for dy in range(3):
            left, middle, right = (
                taps[which][(3 * dy + dx) * count : (3 * dy + dx + 1) * count] for dx in range(3)
            )
            combined.append(
                middle
                + jnp.where(column == 0, 0.0, pltpu.roll(left, 1, 1))
                + jnp.where(column == W - 1, 0.0, pltpu.roll(right, tokens - 1, 1))
            )
        above, middle, below = combined
        part = (
            bases[which]
            + middle
            + jnp.where(token < W, 0.0, pltpu.roll(above, W, 1))
            + jnp.where(token >= tokens - W, 0.0, pltpu.roll(below, tokens - W, 1))
        )
        part_ref[here] = part
        kept = jnp.where(jnp.logical_and(token >= begin, token < end), part, 0.0)
        totals = by_group(jnp.sum(kept, axis=1, keepdims=True))
        squares = by_group(jnp.sum(kept * kept, axis=1, keepdims=True))
        bottom = pltpu.roll(part[:, tokens - 128 :], 2 * W, 1)
        up = pltpu.roll(below[:, :128], 2 * W, 1)
        note = jnp.where(lane < W, part[:, :128], jnp.where(lane < 2 * W, bottom, jnp.where(lane < 3 * W, up, above[:, tokens - 128 :])))
        for copy in range(note_ref.shape[0]):
            note_ref[copy, pl.ds(pl.multiple_of(here * count, 16), count), :] = note.astype(BF16)
        for group in range(len(totals)):
            for kind, value in enumerate((totals[group], squares[group])):
                for piece in range(3):
                    rounded = value.astype(BF16).astype(F32)
                    index = (here * len(totals) + group) * 6 + kind * 3 + piece
                    extra = jnp.where(extra_lane == index, rounded, extra)
                    value = value - rounded
    for copy in range(note_ref.shape[0]):
        note_ref[copy, 2 * count :, :] = extra.astype(BF16)


def finish_kernel(part_ref, notes_ref, gain_ref, mail_ref, *outs, act, lane_of):
    _, count, tokens = part_ref.shape
    mine, _, quarter = spot()
    own_gain = upright([gain_ref[...]])[:, 0:1]
    lane = lanes((count, 128))
    sums = notes_ref[0, 2 * count :].astype(F32)
    for place in range(1, 4):
        sums = sums + notes_ref[place, 2 * count :].astype(F32)
    before = jnp.maximum(quarter - 1, 0)
    after = jnp.minimum(quarter + 1, 3)
    for side in range(2):
        rows = slice(side * count, (side + 1) * count)
        notes = [notes_ref[place, rows].astype(F32) for place in range(4)]
        total = jnp.zeros((count, 1), F32)
        squares = jnp.zeros((count, 1), F32)
        for low in range(3):
            one, two = notes[low], notes[low + 1]
            edges = jnp.where(
                lane < W,
                two + pltpu.roll(one, W, 1),
                jnp.where(lane < 2 * W, one + pltpu.roll(two, 128 - W, 1), 0.0),
            )
            total = total + jnp.sum(edges, axis=1, keepdims=True)
            squares = squares + jnp.sum(edges * edges, axis=1, keepdims=True)
        top = pltpu.roll(notes_ref[before, rows].astype(F32), W, 1)
        low = pltpu.roll(notes_ref[after, rows].astype(F32), W, 1)
        part = part_ref[side]
        value = jnp.concatenate(
            [
                part[:, :128] + jnp.where(lane < jnp.where(quarter > 0, W, 0), top, 0.0),
                part[:, tokens - 128 :] + jnp.where(lane >= jnp.where(quarter < 3, 128 - W, 128), low, 0.0),
            ],
            axis=1,
        )
        totals, squared = by_group(total), by_group(squares)
        at = tokens + lane_of
        gain = jnp.where(side == mine, own_gain, mail_ref[:, at : at + 1])
        pieces = []
        for group in range(len(totals)):
            first = (side * len(totals) + group) * 6
            whole = totals[group] + jnp.sum(sums[0:1, first : first + 3], axis=1, keepdims=True)
            whole_squares = squared[group] + jnp.sum(sums[0:1, first + 3 : first + 6], axis=1, keepdims=True)
            span = slice(group * WIDE, (group + 1) * WIDE)
            pieces.append(scaled(value[span], whole, whole_squares, gain[span]))
        result = jnp.concatenate(pieces, axis=0)
        result = (silu(result) if act else result).astype(BF16)
        for copy in range(outs[0].shape[0]):
            outs[0][copy, side] = result
        if not act:
            outs[1][side] = value


def project_kernel(query_ref, key_ref, value_ref, got_ref, full_ref, q_ref, kv_ref, whole_ref, stack_ref):
    inner = query_ref.shape[0]
    side, _, _ = spot()
    for index, ref in enumerate((query_ref, key_ref, value_ref)):
        stack_ref[index * inner : (index + 1) * inner] = ref[...]
    gather_into(full_ref, whole_ref)
    mixed = both(stack_ref[...], [got_ref[: 3 * inner]], whole_ref)
    for which in range(2):
        here = side if which == 0 else 1 - side
        q_ref[here] = mixed[which][:inner].astype(BF16)
        for copy in range(kv_ref.shape[0]):
            kv_ref[copy, here] = mixed[which][inner:].astype(BF16)


def attend_kernel(q_ref, pairs_ref, out_ref):
    inner = q_ref.shape[1]
    for head in range(2):
        keys = jnp.concatenate([pairs_ref[place, head, :inner] for place in range(4)], axis=1)
        values = jnp.concatenate([pairs_ref[place, head, inner:] for place in range(4)], axis=1)
        scores = lax.dot_general(
            keys, q_ref[head], (((0,), (0,)), ((), ())), preferred_element_type=F32
        ) * (1.0 / math.sqrt(HEAD_DIM))
        raised = jnp.exp(scores - jnp.max(scores, axis=0, keepdims=True))
        weights = (raised * (1.0 / jnp.sum(raised, axis=0, keepdims=True))).astype(BF16)
        mixed = jnp.dot(values, weights, preferred_element_type=F32).astype(BF16)
        for copy in range(out_ref.shape[0]):
            out_ref[copy, head] = mixed


def leave_kernel(weight_ref, got_ref, full_ref, hidden_ref, keep_ref, send_ref, whole_ref, *, at):
    count, depth = weight_ref.shape
    side, _, _ = spot()
    gather_into(full_ref, whole_ref)
    mine, theirs = both(weight_ref[...], [got_ref[at : at + count, :depth]], whole_ref)
    keep_ref[...] = (hidden_ref[side] + mine).astype(BF16)
    send_ref[...] = (hidden_ref[1 - side] + theirs).astype(BF16)


def last_kernel(keep_ref, peer_ref, result_ref):
    span = keep_ref.shape[1]
    side, core, _ = spot()
    part = side ^ core
    for ref, at in ((keep_ref, part), (peer_ref, 1 - part)):
        result_ref[pl.ds(pl.multiple_of(at * span, 16), span), :] = ref[...].astype(F32).T.astype(BF16)


def body(
    latent,
    timestep,
    norm_gain_a,
    conv_weight_a,
    time_weight,
    norm_gain_b,
    conv_weight_b,
    norm_gain_c,
    w_query,
    w_key,
    w_value,
    w_out,
):
    rows, width, count = latent.shape
    tokens = rows * width
    share = tokens // 2
    chs = lax.axis_size("ch")
    place = lax.axis_index("row")
    image_id = place // 2
    inner = w_query.shape[0]

    def tall(weight):
        return jnp.transpose(weight, (1, 2, 0, 3)).reshape(9 * count, C)

    field = ((2, count, share), F32)
    half_chs = chs // 2
    active = ((half_chs, 2, count, share), BF16)
    note = ((4, 2 * count + 16, 128), BF16)
    whole = pltpu.VMEM((C, share), BF16)

    gain_a, gain_b, gain_c = (gain.reshape(1, count) for gain in (norm_gain_a, norm_gain_b, norm_gain_c))
    own_a, own_b = tall(conv_weight_a), tall(conv_weight_b)
    flat = latent.reshape(tokens, count)
    turned, sums, half_a = call(
        enter_kernel,
        [((count, tokens), F32), ((count, 128), F32), ((9 * count, C // 2), BF16)],
        [VM, FAR],
        [pltpu.SemaphoreType.DMA],
        limit=65_500_000,
    )(flat, own_a)
    peer = swapped(sums)
    got_a = from_beside(half_a)
    (spread_a,) = call(first_kernel, [((chs, count, share), BF16)], [VM] * 4)(turned, sums, peer, gain_a)

    full = lax.all_to_all(spread_a, "ch", 0, 0, tiled=True)
    step_value = jnp.sum(jnp.where(jnp.arange(timestep.shape[0]) == image_id, after(timestep, spread_a), 0)).astype(F32)
    half = TDIM // 2
    freqs = jnp.exp(-math.log(10000.0) * jnp.arange(half, dtype=F32) / half)
    angles = step_value * freqs
    sinus = jnp.concatenate([jnp.cos(angles), jnp.sin(angles)])[None, :].astype(BF16)
    (mail,) = call(mail_kernel, [((count, share + 128), F32)], [VM] * 5)(
        time_weight.T, sinus, gain_b, gain_c, after(flat, spread_a)
    )
    mail = crossed(mail)
    got_b = from_beside(after(own_b, spread_a))
    *late, late_out = [after(weight, spread_a) for weight in (w_query, w_key, w_value, w_out)]
    late.append(jnp.pad(late_out, ((0, 0), (0, C - w_out.shape[1]))))
    got_c = from_beside(jnp.concatenate(late, axis=0))
    other_a = swapped(after(got_a, spread_a))

    def conv(limit, full, own, gots, *bases):
        return call(
            functools.partial(conv_kernel, gots=len(gots)),
            [field, note],
            [VM] * (3 + len(gots) + len(bases)),
            [whole],
            limit=limit,
        )(own, *gots, full, mail, *bases)

    def finish(part, notes, gain, act, lane_of, outs):
        return call(
            functools.partial(finish_kernel, act=act, lane_of=lane_of), outs, [VM] * 4
        )(part, notes, gain, mail)

    part_a, note_a = conv(20 * 2**20, full, own_a, [got_a, other_a], time_weight.T, sinus)
    notes_a = image_collect(note_a)
    (spread_b,) = finish(part_a, notes_a, gain_b, True, 1, [active])
    part_b, note_b = conv(65_000_000, column_collect(spread_b), own_b, [got_b], flat)
    notes_b = image_collect(note_b)
    spread_c, hidden_b = finish(part_b, notes_b, gain_c, False, 2, [active, field])
    features = column_collect(after(spread_c, got_c))

    query, key_value = call(
        project_kernel,
        [((2, inner, share), BF16), ((4, 2, 2 * inner, share), BF16)],
        [VM] * 5,
        [whole, pltpu.VMEM((3 * inner, C), BF16)],
    )(w_query, w_key, w_value, got_c, features)
    pairs = image_collect(key_value)
    (heads_out,) = call(attend_kernel, [((half_chs, 2, inner, share), BF16)], [VM] * 2)(query, pairs)
    kept, sent = call(
        functools.partial(leave_kernel, at=3 * inner),
        [((count, share), BF16)] * 2,
        [VM] * 4,
        [pltpu.VMEM((w_out.shape[1], share), BF16)],
    )(w_out, got_c, column_collect(heads_out), hidden_b)
    (result,) = call(last_kernel, [((tokens, count), BF16)], [VM] * 2)(kept, crossed(sent))
    return result.reshape(rows, width, count)


def solution(mesh):
    return jax.shard_map(
        body,
        mesh=mesh,
        in_specs=(
            P("row", None, "ch"),
            P(),
            P("ch"),
            P("ch", None, None, None),
            P(None, "ch"),
            P("ch"),
            P("ch", None, None, None),
            P("ch"),
            P("ch", None),
            P("ch", None),
            P("ch", None),
            P("ch", None),
        ),
        out_specs=P("row", None, "ch"),
        check_vma=False,
    )
```

```python
import functools
import math

import jax
import jax.numpy as jnp
from jax import lax
from jax.experimental import pallas as pl
from jax.experimental.pallas import tpu as pltpu
from jax.sharding import PartitionSpec as P


C = 1280
GROUPS = 32
HEAD_DIM = 64
TDIM = 320
H = 32
W = 32
WIDE = C // GROUPS
MEMBERS = float(H * W * WIDE)
EPS = 1e-06
F32 = jnp.float32
BF16 = jnp.bfloat16

VM = pl.BlockSpec(memory_space=pltpu.VMEM)
FAR = pl.BlockSpec(memory_space=pltpu.HBM)


def call(kernel, outs, specs, scratch=()):
    return pl.pallas_call(
        kernel,
        out_shape=[jax.ShapeDtypeStruct(s, d) for s, d in outs],
        in_specs=specs,
        out_specs=[VM] * len(outs),
        scratch_shapes=list(scratch),
        compiler_params=pltpu.CompilerParams(vmem_limit_bytes=20 * 2**20),
    )


def device(ch, row):
    return ch * lax.axis_size("row") + row


def core_pairs():
    rows, chs = lax.axis_size("row"), lax.axis_size("ch")
    return [(device(k, r), device(k, r ^ 1)) for k in range(chs) for r in range(rows)]


def swapped(value):
    return lax.ppermute(value, ("ch", "row"), core_pairs())


def crossed(value):
    chs = lax.axis_size("ch")
    return lax.ppermute(value, "ch", [(k, (k + chs // 2) % chs) for k in range(chs)])


def from_beside(value, each_core=False):
    rows, chs = lax.axis_size("row"), lax.axis_size("ch")
    wide = 2 if rows % 4 == 0 else 1
    pairs = []
    for k in range(chs):
        for r in range(rows):
            core, high, rest = r % 2, r // 2 % wide, r // (2 * wide)
            side = k // (chs // 2)
            ahead = core == 0 if each_core else side == 1
            x = (2 * high + side + (1 if ahead else -1)) % (2 * wide)
            source = device(x % 2 * (chs // 2) + k % (chs // 2), (rest * wide + x // 2) * 2 + core)
            pairs.append((source, device(k, r)))
    return lax.ppermute(value, ("ch", "row"), pairs)


def spot():
    side = lax.axis_index("ch") // (lax.axis_size("ch") // 2)
    core = lax.axis_index("row") % 2
    return side, core, 2 * core + (side ^ core)


def after(value, first):
    return lax.optimization_barrier((value, first))[0]


def column_collect(spread):
    half = lax.axis_size("ch") // 2
    groups = [list(range(half)), list(range(half, 2 * half))]
    return lax.all_to_all(spread, "ch", 0, 0, tiled=True, axis_index_groups=groups)


def image_collect(spread):
    rows, half = lax.axis_size("row"), lax.axis_size("ch") // 2
    groups = [
        [device(k, r), device(k + half, r), device(k + half, r + 1), device(k, r + 1)]
        for r in range(0, rows, 2)
        for k in range(half)
    ]
    return lax.all_to_all(spread, ("ch", "row"), 0, 0, tiled=True, axis_index_groups=groups)


def lanes(shape):
    return lax.broadcasted_iota(jnp.int32, shape, 1)


def silu(u):
    return u / (1.0 + jnp.exp(-u))


def scaled(value, total, squares, gain):
    mean = total / MEMBERS
    spread = squares / MEMBERS - mean * mean
    return (value - mean) * (lax.rsqrt(spread + EPS) * gain)


def by_group(per_channel):
    return [
        jnp.sum(per_channel[first : first + WIDE], axis=0, keepdims=True)
        for first in range(0, per_channel.shape[0], WIDE)
    ]


def enter_kernel(latent_ref, weight_ref, turned_ref, sums_ref, half_ref, sem):
    _, core, _ = spot()
    depth = half_ref.shape[1]
    columns = pl.ds(pl.multiple_of(core * depth, 128), depth)
    copy = pltpu.make_async_copy(weight_ref.at[:, columns], half_ref, sem)
    copy.start()
    value = latent_ref[...].astype(F32).T
    turned_ref[...] = value
    lane = lanes(sums_ref.shape)
    total = jnp.sum(value, axis=1, keepdims=True)
    squares = jnp.sum(value * value, axis=1, keepdims=True)
    sums_ref[...] = jnp.where(lane == 0, total, jnp.where(lane == 1, squares, 0.0))
    copy.wait()


def upright(rows):
    return jnp.concatenate(rows + [jnp.zeros((8 - len(rows), rows[0].shape[1]), F32)], axis=0).T


def first_kernel(turned_ref, own_ref, peer_ref, gain_ref, active_ref):
    _, core, _ = spot()
    sums = own_ref[...] + peer_ref[...]
    totals, squares = by_group(sums[:, 0:1]), by_group(sums[:, 1:2])
    gain = upright([gain_ref[...]])[:, 0:1]
    pieces = []
    for group in range(len(totals)):
        rows = slice(group * WIDE, (group + 1) * WIDE)
        pieces.append(scaled(turned_ref[rows], totals[group], squares[group], gain[rows]))
    value = silu(jnp.concatenate(pieces, axis=0)).astype(BF16)
    half = value.shape[1] // 2
    each = active_ref.shape[0] // 2
    for copy in range(each):
        active_ref[core * each + copy] = value[:, :half]
        active_ref[(1 - core) * each + copy] = value[:, half:]


def time_of(weight_ref, sinus_ref):
    product = weight_ref[...].astype(F32) * sinus_ref[...].astype(F32)
    return silu(jnp.sum(product, axis=1, keepdims=True))


def turned_share(latent_ref, part, share):
    rows = pl.ds(pl.multiple_of(part * share, 16), share)
    return latent_ref[rows, :].astype(F32).T


def mail_kernel(weight_ref, sinus_ref, gain_b_ref, gain_c_ref, latent_ref, mail_ref):
    side, core, _ = spot()
    share = latent_ref.shape[0] // 2
    lane = lanes((mail_ref.shape[0], 128))
    gains = upright([gain_b_ref[...], gain_c_ref[...]])
    vector = jnp.where(lane == 0, time_of(weight_ref, sinus_ref), 0.0)
    for kind in range(2):
        vector = jnp.where(lane == 1 + kind, gains[:, kind : kind + 1], vector)
    mail_ref[:, :share] = turned_share(latent_ref, 1 - (side ^ core), share)
    mail_ref[:, share:] = vector


def gather_into(full_ref, whole_ref):
    if len(full_ref.shape) == 3:
        whole_ref[...] = full_ref[...].reshape(whole_ref.shape)
        return
    peers, _, count, _ = full_ref.shape
    for side in range(2):
        for peer in range(peers):
            at = (side * peers + peer) * count
            whole_ref[at : at + count] = full_ref[peer, side]


def both(own, gots, whole_ref):
    mine = jnp.dot(own, whole_ref[...], preferred_element_type=F32)
    depth = gots[0].shape[1]
    if len(gots) == 1:
        return mine, jnp.dot(gots[0], whole_ref[...], preferred_element_type=F32)
    _, core, _ = spot()
    near = whole_ref[pl.ds(pl.multiple_of(core * depth, 128), depth), :]
    far = whole_ref[pl.ds(pl.multiple_of((1 - core) * depth, 128), depth), :]
    theirs = jnp.dot(gots[0], near, preferred_element_type=F32)
    return mine, theirs + jnp.dot(gots[1], far, preferred_element_type=F32)


def conv_kernel(own_ref, *refs, gots):
    got_refs, refs = refs[:gots], refs[gots:]
    full_ref, mail_ref, *base_refs, part_ref, note_ref, whole_ref = refs
    _, count, tokens = part_ref.shape
    side, core, quarter = spot()
    token = lanes((count, tokens))
    column = token % W
    lane = lanes((count, 128))
    begin = jnp.where(quarter > 0, W, 0)
    end = jnp.where(quarter < 3, tokens - W, tokens)
    gather_into(full_ref, whole_ref)
    taps = both(own_ref[...], [ref[...] for ref in got_refs], whole_ref)
    if len(base_refs) == 2:
        bases = time_of(*base_refs), mail_ref[:, tokens : tokens + 1]
    else:
        bases = turned_share(base_refs[0], side ^ core, tokens), mail_ref[:, :tokens]
    extra = jnp.zeros((16, 128), F32)
    extra_lane = lanes((16, 128))
    for which in range(2):
        here = side if which == 0 else 1 - side
        combined = []
        for dy in range(3):
            left, middle, right = (
                taps[which][(3 * dy + dx) * count : (3 * dy + dx + 1) * count] for dx in range(3)
            )
            combined.append(
                middle
                + jnp.where(column == 0, 0.0, pltpu.roll(left, 1, 1))
                + jnp.where(column == W - 1, 0.0, pltpu.roll(right, tokens - 1, 1))
            )
        above, middle, below = combined
        part = (
            bases[which]
            + middle
            + jnp.where(token < W, 0.0, pltpu.roll(above, W, 1))
            + jnp.where(token >= tokens - W, 0.0, pltpu.roll(below, tokens - W, 1))
        )
        part_ref[here] = part
        kept = jnp.where(jnp.logical_and(token >= begin, token < end), part, 0.0)
        totals = by_group(jnp.sum(kept, axis=1, keepdims=True))
        squares = by_group(jnp.sum(kept * kept, axis=1, keepdims=True))
        bottom = pltpu.roll(part[:, tokens - 128 :], 2 * W, 1)
        up = pltpu.roll(below[:, :128], 2 * W, 1)
        note = jnp.where(lane < W, part[:, :128], jnp.where(lane < 2 * W, bottom, jnp.where(lane < 3 * W, up, above[:, tokens - 128 :])))
        for copy in range(note_ref.shape[0]):
            note_ref[copy, pl.ds(pl.multiple_of(here * count, 16), count), :] = note.astype(BF16)
        for group in range(len(totals)):
            for kind, value in enumerate((totals[group], squares[group])):
                for piece in range(3):
                    rounded = value.astype(BF16).astype(F32)
                    index = (here * len(totals) + group) * 6 + kind * 3 + piece
                    extra = jnp.where(extra_lane == index, rounded, extra)
                    value = value - rounded
    for copy in range(note_ref.shape[0]):
        note_ref[copy, 2 * count :, :] = extra.astype(BF16)


def finish_kernel(part_ref, notes_ref, gain_ref, mail_ref, *outs, act, lane_of):
    _, count, tokens = part_ref.shape
    mine, _, quarter = spot()
    own_gain = upright([gain_ref[...]])[:, 0:1]
    lane = lanes((count, 128))
    sums = notes_ref[0, 2 * count :].astype(F32)
    for place in range(1, 4):
        sums = sums + notes_ref[place, 2 * count :].astype(F32)
    before = jnp.maximum(quarter - 1, 0)
    after = jnp.minimum(quarter + 1, 3)
    for side in range(2):
        rows = slice(side * count, (side + 1) * count)
        notes = [notes_ref[place, rows].astype(F32) for place in range(4)]
        total = jnp.zeros((count, 1), F32)
        squares = jnp.zeros((count, 1), F32)
        for low in range(3):
            one, two = notes[low], notes[low + 1]
            edges = jnp.where(
                lane < W,
                two + pltpu.roll(one, W, 1),
                jnp.where(lane < 2 * W, one + pltpu.roll(two, 128 - W, 1), 0.0),
            )
            total = total + jnp.sum(edges, axis=1, keepdims=True)
            squares = squares + jnp.sum(edges * edges, axis=1, keepdims=True)
        top = pltpu.roll(notes_ref[before, rows].astype(F32), W, 1)
        low = pltpu.roll(notes_ref[after, rows].astype(F32), W, 1)
        part = part_ref[side]
        value = jnp.concatenate(
            [
                part[:, :128] + jnp.where(lane < jnp.where(quarter > 0, W, 0), top, 0.0),
                part[:, tokens - 128 :] + jnp.where(lane >= jnp.where(quarter < 3, 128 - W, 128), low, 0.0),
            ],
            axis=1,
        )
        totals, squared = by_group(total), by_group(squares)
        at = tokens + lane_of
        gain = jnp.where(side == mine, own_gain, mail_ref[:, at : at + 1])
        pieces = []
        for group in range(len(totals)):
            first = (side * len(totals) + group) * 6
            whole = totals[group] + jnp.sum(sums[0:1, first : first + 3], axis=1, keepdims=True)
            whole_squares = squared[group] + jnp.sum(sums[0:1, first + 3 : first + 6], axis=1, keepdims=True)
            span = slice(group * WIDE, (group + 1) * WIDE)
            pieces.append(scaled(value[span], whole, whole_squares, gain[span]))
        result = jnp.concatenate(pieces, axis=0)
        result = (silu(result) if act else result).astype(BF16)
        for copy in range(outs[0].shape[0]):
            outs[0][copy, side] = result
        if not act:
            outs[1][side] = value


def project_kernel(query_ref, key_ref, value_ref, got_ref, full_ref, q_ref, kv_ref, whole_ref, stack_ref):
    inner = query_ref.shape[0]
    side, _, _ = spot()
    for index, ref in enumerate((query_ref, key_ref, value_ref)):
        stack_ref[index * inner : (index + 1) * inner] = ref[...]
    gather_into(full_ref, whole_ref)
    mixed = both(stack_ref[...], [got_ref[: 3 * inner]], whole_ref)
    for which in range(2):
        here = side if which == 0 else 1 - side
        q_ref[here] = mixed[which][:inner].astype(BF16)
        for copy in range(kv_ref.shape[0]):
            kv_ref[copy, here] = mixed[which][inner:].astype(BF16)


def attend_kernel(q_ref, pairs_ref, out_ref):
    inner = q_ref.shape[1]
    for head in range(2):
        keys = jnp.concatenate([pairs_ref[place, head, :inner] for place in range(4)], axis=1)
        values = jnp.concatenate([pairs_ref[place, head, inner:] for place in range(4)], axis=1)
        scores = lax.dot_general(
            keys, q_ref[head], (((0,), (0,)), ((), ())), preferred_element_type=F32
        ) * (1.0 / math.sqrt(HEAD_DIM))
        raised = jnp.exp(scores - jnp.max(scores, axis=0, keepdims=True))
        weights = (raised * (1.0 / jnp.sum(raised, axis=0, keepdims=True))).astype(BF16)
        mixed = jnp.dot(values, weights, preferred_element_type=F32).astype(BF16)
        for copy in range(out_ref.shape[0]):
            out_ref[copy, head] = mixed


def leave_kernel(weight_ref, got_ref, full_ref, hidden_ref, keep_ref, send_ref, whole_ref, *, at):
    count, depth = weight_ref.shape
    side, _, _ = spot()
    gather_into(full_ref, whole_ref)
    mine, theirs = both(weight_ref[...], [got_ref[at : at + count, :depth]], whole_ref)
    keep_ref[...] = (hidden_ref[side] + mine).astype(BF16)
    send_ref[...] = (hidden_ref[1 - side] + theirs).astype(BF16)


def last_kernel(keep_ref, peer_ref, result_ref):
    span = keep_ref.shape[1]
    side, core, _ = spot()
    part = side ^ core
    for ref, at in ((keep_ref, part), (peer_ref, 1 - part)):
        result_ref[pl.ds(pl.multiple_of(at * span, 16), span), :] = ref[...].astype(F32).T.astype(BF16)


def body(
    latent,
    timestep,
    norm_gain_a,
    conv_weight_a,
    time_weight,
    norm_gain_b,
    conv_weight_b,
    norm_gain_c,
    w_query,
    w_key,
    w_value,
    w_out,
):
    rows, width, count = latent.shape
    tokens = rows * width
    share = tokens // 2
    chs = lax.axis_size("ch")
    place = lax.axis_index("row")
    image_id = place // 2
    inner = w_query.shape[0]

    def tall(weight):
        return jnp.transpose(weight, (1, 2, 0, 3)).reshape(9 * count, C)

    field = ((2, count, share), F32)
    half_chs = chs // 2
    active = ((half_chs, 2, count, share), BF16)
    note = ((4, 2 * count + 16, 128), BF16)
    whole = pltpu.VMEM((C, share), BF16)

    gain_a, gain_b, gain_c = (gain.reshape(1, count) for gain in (norm_gain_a, norm_gain_b, norm_gain_c))
    own_a, own_b = tall(conv_weight_a), tall(conv_weight_b)
    flat = latent.reshape(tokens, count)
    turned, sums, half_a = call(
        enter_kernel,
        [((count, tokens), F32), ((count, 128), F32), ((9 * count, C // 2), BF16)],
        [VM, FAR],
        [pltpu.SemaphoreType.DMA],
    )(flat, own_a)
    peer = swapped(sums)
    got_a = from_beside(half_a, each_core=True)
    (spread_a,) = call(first_kernel, [((chs, count, share), BF16)], [VM] * 4)(turned, sums, peer, gain_a)

    full = lax.all_to_all(spread_a, "ch", 0, 0, tiled=True)
    step_value = jnp.sum(jnp.where(jnp.arange(timestep.shape[0]) == image_id, after(timestep, spread_a), 0)).astype(F32)
    half = TDIM // 2
    freqs = jnp.exp(-math.log(10000.0) * jnp.arange(half, dtype=F32) / half)
    angles = step_value * freqs
    sinus = jnp.concatenate([jnp.cos(angles), jnp.sin(angles)])[None, :].astype(BF16)
    (mail,) = call(mail_kernel, [((count, share + 128), F32)], [VM] * 5)(
        time_weight.T, sinus, gain_b, gain_c, after(flat, spread_a)
    )
    mail = crossed(mail)
    got_b = from_beside(after(own_b, spread_a))
    other_a = swapped(after(got_a, spread_a))

    def conv(full, own, gots, *bases):
        return call(
            functools.partial(conv_kernel, gots=len(gots)),
            [field, note],
            [VM] * (3 + len(gots) + len(bases)),
            [whole],
        )(own, *gots, full, mail, *bases)

    def finish(part, notes, gain, act, lane_of, outs):
        return call(
            functools.partial(finish_kernel, act=act, lane_of=lane_of), outs, [VM] * 4
        )(part, notes, gain, mail)

    part_a, note_a = conv(full, own_a, [got_a, other_a], time_weight.T, sinus)
    notes_a = image_collect(note_a)
    (spread_b,) = finish(part_a, notes_a, gain_b, True, 1, [active])
    full_b = column_collect(spread_b)
    *late, late_out = [after(weight, spread_b) for weight in (w_query, w_key, w_value, w_out)]
    late.append(jnp.pad(late_out, ((0, 0), (0, C - w_out.shape[1]))))
    got_c = from_beside(jnp.concatenate(late, axis=0))
    part_b, note_b = conv(full_b, own_b, [got_b], flat)
    notes_b = image_collect(note_b)
    spread_c, hidden_b = finish(part_b, notes_b, gain_c, False, 2, [active, field])
    features = column_collect(after(spread_c, got_c))

    query, key_value = call(
        project_kernel,
        [((2, inner, share), BF16), ((4, 2, 2 * inner, share), BF16)],
        [VM] * 5,
        [whole, pltpu.VMEM((3 * inner, C), BF16)],
    )(w_query, w_key, w_value, got_c, features)
    pairs = image_collect(key_value)
    (heads_out,) = call(attend_kernel, [((half_chs, 2, inner, share), BF16)], [VM] * 2)(query, pairs)
    kept, sent = call(
        functools.partial(leave_kernel, at=3 * inner),
        [((count, share), BF16)] * 2,
        [VM] * 4,
        [pltpu.VMEM((w_out.shape[1], share), BF16)],
    )(w_out, got_c, column_collect(heads_out), hidden_b)
    (result,) = call(last_kernel, [((tokens, count), BF16)], [VM] * 2)(kept, crossed(sent))
    return result.reshape(rows, width, count)


def solution(mesh):
    return jax.shard_map(
        body,
        mesh=mesh,
        in_specs=(
            P("row", None, "ch"),
            P(),
            P("ch"),
            P("ch", None, None, None),
            P(None, "ch"),
            P("ch"),
            P("ch", None, None, None),
            P("ch"),
            P("ch", None),
            P("ch", None),
            P("ch", None),
            P("ch", None),
        ),
        out_specs=P("row", None, "ch"),
        check_vma=False,
    )
```

```python
import functools
import math

import jax
import jax.numpy as jnp
from jax import lax
from jax.experimental import pallas as pl
from jax.experimental.pallas import tpu as pltpu
from jax.sharding import PartitionSpec as P


C = 1280
GROUPS = 32
HEAD_DIM = 64
TDIM = 320
H = 32
W = 32
WIDE = C // GROUPS
MEMBERS = float(H * W * WIDE)
EPS = 1e-06
F32 = jnp.float32
BF16 = jnp.bfloat16

VM = pl.BlockSpec(memory_space=pltpu.VMEM)
ENTER_LIMIT = 56_000_000
CONV_LIMIT = 54_300_000
FAR = pl.BlockSpec(memory_space=pltpu.HBM)


def call(kernel, outs, specs, scratch=(), limit=20 * 2**20):
    return pl.pallas_call(
        kernel,
        out_shape=[jax.ShapeDtypeStruct(s, d) for s, d in outs],
        in_specs=specs,
        out_specs=[VM] * len(outs),
        scratch_shapes=list(scratch),
        compiler_params=pltpu.CompilerParams(vmem_limit_bytes=limit),
    )


def device(ch, row):
    return ch * lax.axis_size("row") + row


def core_pairs():
    rows, chs = lax.axis_size("row"), lax.axis_size("ch")
    return [(device(k, r), device(k, r ^ 1)) for k in range(chs) for r in range(rows)]


def swapped(value):
    return lax.ppermute(value, ("ch", "row"), core_pairs())


def crossed(value):
    chs = lax.axis_size("ch")
    return lax.ppermute(value, "ch", [(k, (k + chs // 2) % chs) for k in range(chs)])


def from_beside(value, each_core=False):
    rows, chs = lax.axis_size("row"), lax.axis_size("ch")
    wide = 2 if rows % 4 == 0 else 1
    pairs = []
    for k in range(chs):
        for r in range(rows):
            core, high, rest = r % 2, r // 2 % wide, r // (2 * wide)
            side = k // (chs // 2)
            ahead = core == 0 if each_core else side == 1
            x = (2 * high + side + (1 if ahead else -1)) % (2 * wide)
            source = device(x % 2 * (chs // 2) + k % (chs // 2), (rest * wide + x // 2) * 2 + core)
            pairs.append((source, device(k, r)))
    return lax.ppermute(value, ("ch", "row"), pairs)


def spot():
    side = lax.axis_index("ch") // (lax.axis_size("ch") // 2)
    core = lax.axis_index("row") % 2
    return side, core, 2 * core + (side ^ core)


def after(value, first):
    return lax.optimization_barrier((value, first))[0]


def column_collect(spread):
    half = lax.axis_size("ch") // 2
    groups = [list(range(half)), list(range(half, 2 * half))]
    return lax.all_to_all(spread, "ch", 0, 0, tiled=True, axis_index_groups=groups)


def image_collect(spread):
    rows, half = lax.axis_size("row"), lax.axis_size("ch") // 2
    groups = [
        [device(k, r), device(k + half, r), device(k + half, r + 1), device(k, r + 1)]
        for r in range(0, rows, 2)
        for k in range(half)
    ]
    return lax.all_to_all(spread, ("ch", "row"), 0, 0, tiled=True, axis_index_groups=groups)


def lanes(shape):
    return lax.broadcasted_iota(jnp.int32, shape, 1)


def silu(u):
    return u / (1.0 + jnp.exp(-u))


def scaled(value, total, squares, gain):
    mean = total / MEMBERS
    spread = squares / MEMBERS - mean * mean
    return (value - mean) * (lax.rsqrt(spread + EPS) * gain)


def by_group(per_channel):
    return [
        jnp.sum(per_channel[first : first + WIDE], axis=0, keepdims=True)
        for first in range(0, per_channel.shape[0], WIDE)
    ]


def enter_kernel(latent_ref, weight_ref, turned_ref, sums_ref, half_ref, sem):
    _, core, _ = spot()
    depth = half_ref.shape[1]
    columns = pl.ds(pl.multiple_of(core * depth, 128), depth)
    copy = pltpu.make_async_copy(weight_ref.at[:, columns], half_ref, sem)
    copy.start()
    value = latent_ref[...].astype(F32).T
    turned_ref[...] = value
    lane = lanes(sums_ref.shape)
    total = jnp.sum(value, axis=1, keepdims=True)
    squares = jnp.sum(value * value, axis=1, keepdims=True)
    sums_ref[...] = jnp.where(lane == 0, total, jnp.where(lane == 1, squares, 0.0))
    copy.wait()


def upright(rows):
    return jnp.concatenate(rows + [jnp.zeros((8 - len(rows), rows[0].shape[1]), F32)], axis=0).T


def first_kernel(turned_ref, own_ref, peer_ref, gain_ref, active_ref):
    _, core, _ = spot()
    sums = own_ref[...] + peer_ref[...]
    totals, squares = by_group(sums[:, 0:1]), by_group(sums[:, 1:2])
    gain = upright([gain_ref[...]])[:, 0:1]
    pieces = []
    for group in range(len(totals)):
        rows = slice(group * WIDE, (group + 1) * WIDE)
        pieces.append(scaled(turned_ref[rows], totals[group], squares[group], gain[rows]))
    value = silu(jnp.concatenate(pieces, axis=0)).astype(BF16)
    half = value.shape[1] // 2
    each = active_ref.shape[0] // 2
    for copy in range(each):
        active_ref[core * each + copy] = value[:, :half]
        active_ref[(1 - core) * each + copy] = value[:, half:]


def time_of(weight_ref, sinus_ref):
    product = weight_ref[...].astype(F32) * sinus_ref[...].astype(F32)
    return silu(jnp.sum(product, axis=1, keepdims=True))


def turned_share(latent_ref, part, share):
    rows = pl.ds(pl.multiple_of(part * share, 16), share)
    return latent_ref[rows, :].astype(F32).T


def mail_kernel(weight_ref, sinus_ref, gain_b_ref, gain_c_ref, latent_ref, mail_ref):
    side, core, _ = spot()
    share = latent_ref.shape[0] // 2
    lane = lanes((mail_ref.shape[0], 128))
    gains = upright([gain_b_ref[...], gain_c_ref[...]])
    vector = jnp.where(lane == 0, time_of(weight_ref, sinus_ref), 0.0)
    for kind in range(2):
        vector = jnp.where(lane == 1 + kind, gains[:, kind : kind + 1], vector)
    mail_ref[:, :share] = turned_share(latent_ref, 1 - (side ^ core), share)
    mail_ref[:, share:] = vector


def gather_into(full_ref, whole_ref):
    if len(full_ref.shape) == 3:
        whole_ref[...] = full_ref[...].reshape(whole_ref.shape)
        return
    peers, _, count, _ = full_ref.shape
    for side in range(2):
        for peer in range(peers):
            at = (side * peers + peer) * count
            whole_ref[at : at + count] = full_ref[peer, side]


def arrived(ref, held_ref, sem):
    pltpu.make_async_copy(ref, held_ref, sem).wait()
    return held_ref[...]


def both(own, gots, whole_ref):
    mine = jnp.dot(own, whole_ref[...], preferred_element_type=F32)
    depth = gots[0].shape[1]
    if len(gots) == 1:
        return mine, jnp.dot(gots[0], whole_ref[...], preferred_element_type=F32)
    _, core, _ = spot()
    near = whole_ref[pl.ds(pl.multiple_of(core * depth, 128), depth), :]
    far = whole_ref[pl.ds(pl.multiple_of((1 - core) * depth, 128), depth), :]
    theirs = jnp.dot(gots[0], near, preferred_element_type=F32)
    return mine, theirs + jnp.dot(gots[1], far, preferred_element_type=F32)


def conv_kernel(own_ref, *refs, gots, copied):
    got_refs, refs = refs[:gots], refs[gots:]
    full_ref, mail_ref, *base_refs, part_ref, note_ref, whole_ref = refs[: len(refs) - 3 * copied]
    if copied:
        weights = list(zip((own_ref, got_refs[0]), refs[-3:-1], (refs[-1].at[0], refs[-1].at[1])))
        for ref, held_ref, sem in weights:
            pltpu.make_async_copy(ref, held_ref, sem).start()
    _, count, tokens = part_ref.shape
    side, core, quarter = spot()
    token = lanes((count, tokens))
    column = token % W
    lane = lanes((count, 128))
    begin = jnp.where(quarter > 0, W, 0)
    end = jnp.where(quarter < 3, tokens - W, tokens)
    gather_into(full_ref, whole_ref)
    if copied:
        taps = [jnp.dot(arrived(*each), whole_ref[...], preferred_element_type=F32) for each in weights]
    else:
        taps = both(own_ref[...], [ref[...] for ref in got_refs], whole_ref)
    if len(base_refs) == 2:
        bases = time_of(*base_refs), mail_ref[:, tokens : tokens + 1]
    else:
        bases = turned_share(base_refs[0], side ^ core, tokens), mail_ref[:, :tokens]
    extra = jnp.zeros((16, 128), F32)
    extra_lane = lanes((16, 128))
    for which in range(2):
        here = side if which == 0 else 1 - side
        combined = []
        for dy in range(3):
            left, middle, right = (
                taps[which][(3 * dy + dx) * count : (3 * dy + dx + 1) * count] for dx in range(3)
            )
            combined.append(
                middle
                + jnp.where(column == 0, 0.0, pltpu.roll(left, 1, 1))
                + jnp.where(column == W - 1, 0.0, pltpu.roll(right, tokens - 1, 1))
            )
        above, middle, below = combined
        part = (
            bases[which]
            + middle
            + jnp.where(token < W, 0.0, pltpu.roll(above, W, 1))
            + jnp.where(token >= tokens - W, 0.0, pltpu.roll(below, tokens - W, 1))
        )
        part_ref[here] = part
        kept = jnp.where(jnp.logical_and(token >= begin, token < end), part, 0.0)
        totals = by_group(jnp.sum(kept, axis=1, keepdims=True))
        squares = by_group(jnp.sum(kept * kept, axis=1, keepdims=True))
        bottom = pltpu.roll(part[:, tokens - 128 :], 2 * W, 1)
        up = pltpu.roll(below[:, :128], 2 * W, 1)
        note = jnp.where(lane < W, part[:, :128], jnp.where(lane < 2 * W, bottom, jnp.where(lane < 3 * W, up, above[:, tokens - 128 :])))
        for copy in range(note_ref.shape[0]):
            note_ref[copy, pl.ds(pl.multiple_of(here * count, 16), count), :] = note.astype(BF16)
        for group in range(len(totals)):
            for kind, value in enumerate((totals[group], squares[group])):
                for piece in range(3):
                    rounded = value.astype(BF16).astype(F32)
                    index = (here * len(totals) + group) * 6 + kind * 3 + piece
                    extra = jnp.where(extra_lane == index, rounded, extra)
                    value = value - rounded
    for copy in range(note_ref.shape[0]):
        note_ref[copy, 2 * count :, :] = extra.astype(BF16)


def finish_kernel(part_ref, notes_ref, gain_ref, mail_ref, *outs, act, lane_of):
    _, count, tokens = part_ref.shape
    mine, _, quarter = spot()
    own_gain = upright([gain_ref[...]])[:, 0:1]
    lane = lanes((count, 128))
    sums = notes_ref[0, 2 * count :].astype(F32)
    for place in range(1, 4):
        sums = sums + notes_ref[place, 2 * count :].astype(F32)
    before = jnp.maximum(quarter - 1, 0)
    after = jnp.minimum(quarter + 1, 3)
    for side in range(2):
        rows = slice(side * count, (side + 1) * count)
        notes = [notes_ref[place, rows].astype(F32) for place in range(4)]
        total = jnp.zeros((count, 1), F32)
        squares = jnp.zeros((count, 1), F32)
        for low in range(3):
            one, two = notes[low], notes[low + 1]
            edges = jnp.where(
                lane < W,
                two + pltpu.roll(one, W, 1),
                jnp.where(lane < 2 * W, one + pltpu.roll(two, 128 - W, 1), 0.0),
            )
            total = total + jnp.sum(edges, axis=1, keepdims=True)
            squares = squares + jnp.sum(edges * edges, axis=1, keepdims=True)
        top = pltpu.roll(notes_ref[before, rows].astype(F32), W, 1)
        low = pltpu.roll(notes_ref[after, rows].astype(F32), W, 1)
        part = part_ref[side]
        value = jnp.concatenate(
            [
                part[:, :128] + jnp.where(lane < jnp.where(quarter > 0, W, 0), top, 0.0),
                part[:, tokens - 128 :] + jnp.where(lane >= jnp.where(quarter < 3, 128 - W, 128), low, 0.0),
            ],
            axis=1,
        )
        totals, squared = by_group(total), by_group(squares)
        at = tokens + lane_of
        gain = jnp.where(side == mine, own_gain, mail_ref[:, at : at + 1])
        pieces = []
        for group in range(len(totals)):
            first = (side * len(totals) + group) * 6
            whole = totals[group] + jnp.sum(sums[0:1, first : first + 3], axis=1, keepdims=True)
            whole_squares = squared[group] + jnp.sum(sums[0:1, first + 3 : first + 6], axis=1, keepdims=True)
            span = slice(group * WIDE, (group + 1) * WIDE)
            pieces.append(scaled(value[span], whole, whole_squares, gain[span]))
        result = jnp.concatenate(pieces, axis=0)
        result = (silu(result) if act else result).astype(BF16)
        for copy in range(outs[0].shape[0]):
            outs[0][copy, side] = result
        if not act:
            outs[1][side] = value


def project_kernel(query_ref, key_ref, value_ref, got_ref, full_ref, q_ref, kv_ref, whole_ref, stack_ref):
    inner = query_ref.shape[0]
    side, _, _ = spot()
    for index, ref in enumerate((query_ref, key_ref, value_ref)):
        stack_ref[index * inner : (index + 1) * inner] = ref[...]
    gather_into(full_ref, whole_ref)
    mixed = both(stack_ref[...], [got_ref[: 3 * inner]], whole_ref)
    for which in range(2):
        here = side if which == 0 else 1 - side
        q_ref[here] = mixed[which][:inner].astype(BF16)
        for copy in range(kv_ref.shape[0]):
            kv_ref[copy, here] = mixed[which][inner:].astype(BF16)


def attend_kernel(q_ref, pairs_ref, out_ref):
    inner = q_ref.shape[1]
    for head in range(2):
        keys = jnp.concatenate([pairs_ref[place, head, :inner] for place in range(4)], axis=1)
        values = jnp.concatenate([pairs_ref[place, head, inner:] for place in range(4)], axis=1)
        scores = lax.dot_general(
            keys, q_ref[head], (((0,), (0,)), ((), ())), preferred_element_type=F32
        ) * (1.0 / math.sqrt(HEAD_DIM))
        raised = jnp.exp(scores - jnp.max(scores, axis=0, keepdims=True))
        weights = (raised * (1.0 / jnp.sum(raised, axis=0, keepdims=True))).astype(BF16)
        mixed = jnp.dot(values, weights, preferred_element_type=F32).astype(BF16)
        for copy in range(out_ref.shape[0]):
            out_ref[copy, head] = mixed


def leave_kernel(weight_ref, got_ref, full_ref, hidden_ref, keep_ref, send_ref, whole_ref, *, at):
    count, depth = weight_ref.shape
    side, _, _ = spot()
    gather_into(full_ref, whole_ref)
    mine, theirs = both(weight_ref[...], [got_ref[at : at + count, :depth]], whole_ref)
    keep_ref[...] = (hidden_ref[side] + mine).astype(BF16)
    send_ref[...] = (hidden_ref[1 - side] + theirs).astype(BF16)


def last_kernel(keep_ref, peer_ref, result_ref):
    span = keep_ref.shape[1]
    side, core, _ = spot()
    part = side ^ core
    for ref, at in ((keep_ref, part), (peer_ref, 1 - part)):
        result_ref[pl.ds(pl.multiple_of(at * span, 16), span), :] = ref[...].astype(F32).T.astype(BF16)


def body(
    latent,
    timestep,
    norm_gain_a,
    conv_weight_a,
    time_weight,
    norm_gain_b,
    conv_weight_b,
    norm_gain_c,
    w_query,
    w_key,
    w_value,
    w_out,
):
    rows, width, count = latent.shape
    tokens = rows * width
    share = tokens // 2
    chs = lax.axis_size("ch")
    place = lax.axis_index("row")
    image_id = place // 2
    inner = w_query.shape[0]

    def tall(weight):
        return jnp.transpose(weight, (1, 2, 0, 3)).reshape(9 * count, C)

    field = ((2, count, share), F32)
    half_chs = chs // 2
    active = ((half_chs, 2, count, share), BF16)
    note = ((4, 2 * count + 16, 128), BF16)
    whole = pltpu.VMEM((C, share), BF16)

    gain_a, gain_b, gain_c = (gain.reshape(1, count) for gain in (norm_gain_a, norm_gain_b, norm_gain_c))
    own_a, own_b = tall(conv_weight_a), tall(conv_weight_b)
    flat = latent.reshape(tokens, count)
    turned, sums, half_a = call(
        enter_kernel,
        [((count, tokens), F32), ((count, 128), F32), ((9 * count, C // 2), BF16)],
        [VM, FAR],
        [pltpu.SemaphoreType.DMA],
        limit=ENTER_LIMIT,
    )(flat, own_a)
    peer = swapped(sums)
    got_a = from_beside(half_a, each_core=True)
    (spread_a,) = call(first_kernel, [((chs, count, share), BF16)], [VM] * 4)(turned, sums, peer, gain_a)

    full = lax.all_to_all(spread_a, "ch", 0, 0, tiled=True)
    step_value = jnp.sum(jnp.where(jnp.arange(timestep.shape[0]) == image_id, after(timestep, spread_a), 0)).astype(F32)
    half = TDIM // 2
    freqs = jnp.exp(-math.log(10000.0) * jnp.arange(half, dtype=F32) / half)
    angles = step_value * freqs
    sinus = jnp.concatenate([jnp.cos(angles), jnp.sin(angles)])[None, :].astype(BF16)
    (mail,) = call(mail_kernel, [((count, share + 128), F32)], [VM] * 5)(
        time_weight.T, sinus, gain_b, gain_c, after(flat, spread_a)
    )
    mail = crossed(mail)
    got_b = from_beside(after(own_b, spread_a))
    other_a = swapped(after(got_a, spread_a))

    def conv(full, own, gots, *bases, copied=False):
        held = [pltpu.VMEM(own.shape, BF16)] * 2 + [pltpu.SemaphoreType.DMA((2,))]
        return call(
            functools.partial(conv_kernel, gots=len(gots), copied=int(copied)),
            [field, note],
            [FAR if copied else VM] * (1 + len(gots)) + [VM] * (2 + len(bases)),
            [whole] + held * copied,
            limit=CONV_LIMIT if copied else 20 * 2**20,
        )(own, *gots, full, mail, *bases)

    def finish(part, notes, gain, act, lane_of, outs):
        return call(
            functools.partial(finish_kernel, act=act, lane_of=lane_of), outs, [VM] * 4
        )(part, notes, gain, mail)

    part_a, note_a = conv(full, own_a, [got_a, other_a], time_weight.T, sinus)
    notes_a = image_collect(note_a)
    (spread_b,) = finish(part_a, notes_a, gain_b, True, 1, [active])
    full_b = column_collect(spread_b)
    *late, late_out = [after(weight, spread_b) for weight in (w_query, w_key, w_value, w_out)]
    late.append(jnp.pad(late_out, ((0, 0), (0, C - w_out.shape[1]))))
    got_c = from_beside(jnp.concatenate(late, axis=0))
    part_b, note_b = conv(full_b, own_b, [got_b], flat, copied=True)
    notes_b = image_collect(note_b)
    spread_c, hidden_b = finish(part_b, notes_b, gain_c, False, 2, [active, field])
    features = column_collect(after(spread_c, got_c))

    query, key_value = call(
        project_kernel,
        [((2, inner, share), BF16), ((4, 2, 2 * inner, share), BF16)],
        [VM] * 5,
        [whole, pltpu.VMEM((3 * inner, C), BF16)],
    )(w_query, w_key, w_value, got_c, features)
    pairs = image_collect(key_value)
    (heads_out,) = call(attend_kernel, [((half_chs, 2, inner, share), BF16)], [VM] * 2)(query, pairs)
    kept, sent = call(
        functools.partial(leave_kernel, at=3 * inner),
        [((count, share), BF16)] * 2,
        [VM] * 4,
        [pltpu.VMEM((w_out.shape[1], share), BF16)],
    )(w_out, got_c, column_collect(heads_out), hidden_b)
    (result,) = call(last_kernel, [((tokens, count), BF16)], [VM] * 2)(kept, crossed(sent))
    return result.reshape(rows, width, count)


def solution(mesh):
    return jax.shard_map(
        body,
        mesh=mesh,
        in_specs=(
            P("row", None, "ch"),
            P(),
            P("ch"),
            P("ch", None, None, None),
            P(None, "ch"),
            P("ch"),
            P("ch", None, None, None),
            P("ch"),
            P("ch", None),
            P("ch", None),
            P("ch", None),
            P("ch", None),
        ),
        out_specs=P("row", None, "ch"),
        check_vma=False,
    )
```

```python
import functools
import math

import jax
import jax.numpy as jnp
from jax import lax
from jax.experimental import pallas as pl
from jax.experimental.pallas import tpu as pltpu
from jax.sharding import PartitionSpec as P


C = 1280
GROUPS = 32
HEAD_DIM = 64
TDIM = 320
H = 32
W = 32
WIDE = C // GROUPS
MEMBERS = float(H * W * WIDE)
EPS = 1e-06
F32 = jnp.float32
BF16 = jnp.bfloat16

VM = pl.BlockSpec(memory_space=pltpu.VMEM)
ENTER_LIMIT = 56_000_000
CONV_LIMIT = 54_300_000
FAR = pl.BlockSpec(memory_space=pltpu.HBM)


def call(kernel, outs, specs, scratch=(), limit=20 * 2**20):
    return pl.pallas_call(
        kernel,
        out_shape=[jax.ShapeDtypeStruct(s, d) for s, d in outs],
        in_specs=specs,
        out_specs=[VM] * len(outs),
        scratch_shapes=list(scratch),
        compiler_params=pltpu.CompilerParams(vmem_limit_bytes=limit),
    )


def device(ch, row):
    return ch * lax.axis_size("row") + row


def core_pairs():
    rows, chs = lax.axis_size("row"), lax.axis_size("ch")
    return [(device(k, r), device(k, r ^ 1)) for k in range(chs) for r in range(rows)]


def swapped(value):
    return lax.ppermute(value, ("ch", "row"), core_pairs())


def crossed(value):
    chs = lax.axis_size("ch")
    return lax.ppermute(value, "ch", [(k, (k + chs // 2) % chs) for k in range(chs)])


def from_beside(value, each_core=False):
    rows, chs = lax.axis_size("row"), lax.axis_size("ch")
    wide = 2 if rows % 4 == 0 else 1
    pairs = []
    for k in range(chs):
        for r in range(rows):
            core, high, rest = r % 2, r // 2 % wide, r // (2 * wide)
            side = k // (chs // 2)
            ahead = core == 0 if each_core else side == 1
            x = (2 * high + side + (1 if ahead else -1)) % (2 * wide)
            source = device(x % 2 * (chs // 2) + k % (chs // 2), (rest * wide + x // 2) * 2 + core)
            pairs.append((source, device(k, r)))
    return lax.ppermute(value, ("ch", "row"), pairs)


def spot():
    side = lax.axis_index("ch") // (lax.axis_size("ch") // 2)
    core = lax.axis_index("row") % 2
    return side, core, 2 * core + (side ^ core)


def after(value, first):
    return lax.optimization_barrier((value, first))[0]


def column_collect(spread):
    half = lax.axis_size("ch") // 2
    groups = [list(range(half)), list(range(half, 2 * half))]
    return lax.all_to_all(spread, "ch", 0, 0, tiled=True, axis_index_groups=groups)


def image_collect(spread):
    rows, half = lax.axis_size("row"), lax.axis_size("ch") // 2
    groups = [
        [device(k, r), device(k + half, r), device(k + half, r + 1), device(k, r + 1)]
        for r in range(0, rows, 2)
        for k in range(half)
    ]
    return lax.all_to_all(spread, ("ch", "row"), 0, 0, tiled=True, axis_index_groups=groups)


def lanes(shape):
    return lax.broadcasted_iota(jnp.int32, shape, 1)


def silu(u):
    return u / (1.0 + jnp.exp(-u))


def scaled(value, total, squares, gain):
    mean = total / MEMBERS
    spread = squares / MEMBERS - mean * mean
    return (value - mean) * (lax.rsqrt(spread + EPS) * gain)


def by_group(per_channel):
    return [
        jnp.sum(per_channel[first : first + WIDE], axis=0, keepdims=True)
        for first in range(0, per_channel.shape[0], WIDE)
    ]


def enter_kernel(latent_ref, weight_ref, turned_ref, sums_ref, half_ref, sem):
    _, core, _ = spot()
    depth = half_ref.shape[1]
    columns = pl.ds(pl.multiple_of(core * depth, 128), depth)
    copy = pltpu.make_async_copy(weight_ref.at[:, columns], half_ref, sem)
    copy.start()
    value = latent_ref[...].astype(F32).T
    turned_ref[...] = value
    lane = lanes(sums_ref.shape)
    total = jnp.sum(value, axis=1, keepdims=True)
    squares = jnp.sum(value * value, axis=1, keepdims=True)
    sums_ref[...] = jnp.where(lane == 0, total, jnp.where(lane == 1, squares, 0.0))
    copy.wait()


def upright(rows):
    return jnp.concatenate(rows + [jnp.zeros((8 - len(rows), rows[0].shape[1]), F32)], axis=0).T


def first_kernel(turned_ref, own_ref, peer_ref, gain_ref, active_ref):
    _, core, _ = spot()
    sums = own_ref[...] + peer_ref[...]
    totals, squares = by_group(sums[:, 0:1]), by_group(sums[:, 1:2])
    gain = upright([gain_ref[...]])[:, 0:1]
    pieces = []
    for group in range(len(totals)):
        rows = slice(group * WIDE, (group + 1) * WIDE)
        pieces.append(scaled(turned_ref[rows], totals[group], squares[group], gain[rows]))
    value = silu(jnp.concatenate(pieces, axis=0)).astype(BF16)
    half = value.shape[1] // 2
    each = active_ref.shape[0] // 2
    for copy in range(each):
        active_ref[core * each + copy] = value[:, :half]
        active_ref[(1 - core) * each + copy] = value[:, half:]


def time_of(weight_ref, sinus_ref):
    product = weight_ref[...].astype(F32) * sinus_ref[...].astype(F32)
    return silu(jnp.sum(product, axis=1, keepdims=True))


def turned_share(latent_ref, part, share):
    rows = pl.ds(pl.multiple_of(part * share, 16), share)
    return latent_ref[rows, :].astype(F32).T


def mail_kernel(weight_ref, sinus_ref, gain_b_ref, gain_c_ref, latent_ref, mail_ref):
    side, core, _ = spot()
    share = latent_ref.shape[0] // 2
    lane = lanes((mail_ref.shape[0], 128))
    gains = upright([gain_b_ref[...], gain_c_ref[...]])
    vector = jnp.where(lane == 0, time_of(weight_ref, sinus_ref), 0.0)
    for kind in range(2):
        vector = jnp.where(lane == 1 + kind, gains[:, kind : kind + 1], vector)
    mail_ref[:, :share] = turned_share(latent_ref, 1 - (side ^ core), share)
    mail_ref[:, share:] = vector


def gather_into(full_ref, whole_ref):
    if len(full_ref.shape) == 3:
        whole_ref[...] = full_ref[...].reshape(whole_ref.shape)
        return
    peers, _, count, _ = full_ref.shape
    for side in range(2):
        for peer in range(peers):
            at = (side * peers + peer) * count
            whole_ref[at : at + count] = full_ref[peer, side]


def arrived(ref, held_ref, sem):
    pltpu.make_async_copy(ref, held_ref, sem).wait()
    return held_ref[...]


def both(own_ref, halves, whole_ref):
    mine = jnp.dot(own_ref[...], whole_ref[...], preferred_element_type=F32)
    _, core, _ = spot()
    theirs = 0.0
    for half, index in zip(halves, (core, 1 - core)):
        got = arrived(*half)
        depth = got.shape[1]
        rows = pl.ds(pl.multiple_of(index * depth, 128), depth)
        theirs = theirs + jnp.dot(got, whole_ref[rows, :], preferred_element_type=F32)
    return mine, theirs


def pair(own, got, whole_ref):
    return [jnp.dot(weight, whole_ref[...], preferred_element_type=F32) for weight in (own, got)]


def conv_kernel(own_ref, *refs, gots, copied):
    got_refs, refs = refs[:gots], refs[gots:]
    full_ref, mail_ref, *base_refs, part_ref, note_ref, whole_ref = refs[:-3]
    fetched = ((own_ref,) if copied else ()) + tuple(got_refs)
    weights = list(zip(fetched, refs[-3:-1], (refs[-1].at[0], refs[-1].at[1])))
    for ref, held_ref, sem in weights:
        pltpu.make_async_copy(ref, held_ref, sem).start()
    _, count, tokens = part_ref.shape
    side, core, quarter = spot()
    token = lanes((count, tokens))
    column = token % W
    lane = lanes((count, 128))
    begin = jnp.where(quarter > 0, W, 0)
    end = jnp.where(quarter < 3, tokens - W, tokens)
    gather_into(full_ref, whole_ref)
    if copied:
        taps = [jnp.dot(arrived(*each), whole_ref[...], preferred_element_type=F32) for each in weights]
    else:
        taps = both(own_ref, weights, whole_ref)
    if len(base_refs) == 2:
        bases = time_of(*base_refs), mail_ref[:, tokens : tokens + 1]
    else:
        bases = turned_share(base_refs[0], side ^ core, tokens), mail_ref[:, :tokens]
    extra = jnp.zeros((16, 128), F32)
    extra_lane = lanes((16, 128))
    for which in range(2):
        here = side if which == 0 else 1 - side
        combined = []
        for dy in range(3):
            left, middle, right = (
                taps[which][(3 * dy + dx) * count : (3 * dy + dx + 1) * count] for dx in range(3)
            )
            combined.append(
                middle
                + jnp.where(column == 0, 0.0, pltpu.roll(left, 1, 1))
                + jnp.where(column == W - 1, 0.0, pltpu.roll(right, tokens - 1, 1))
            )
        above, middle, below = combined
        part = (
            bases[which]
            + middle
            + jnp.where(token < W, 0.0, pltpu.roll(above, W, 1))
            + jnp.where(token >= tokens - W, 0.0, pltpu.roll(below, tokens - W, 1))
        )
        part_ref[here] = part
        kept = jnp.where(jnp.logical_and(token >= begin, token < end), part, 0.0)
        totals = by_group(jnp.sum(kept, axis=1, keepdims=True))
        squares = by_group(jnp.sum(kept * kept, axis=1, keepdims=True))
        bottom = pltpu.roll(part[:, tokens - 128 :], 2 * W, 1)
        up = pltpu.roll(below[:, :128], 2 * W, 1)
        note = jnp.where(lane < W, part[:, :128], jnp.where(lane < 2 * W, bottom, jnp.where(lane < 3 * W, up, above[:, tokens - 128 :])))
        for copy in range(note_ref.shape[0]):
            note_ref[copy, pl.ds(pl.multiple_of(here * count, 16), count), :] = note.astype(BF16)
        for group in range(len(totals)):
            for kind, value in enumerate((totals[group], squares[group])):
                for piece in range(3):
                    rounded = value.astype(BF16).astype(F32)
                    index = (here * len(totals) + group) * 6 + kind * 3 + piece
                    extra = jnp.where(extra_lane == index, rounded, extra)
                    value = value - rounded
    for copy in range(note_ref.shape[0]):
        note_ref[copy, 2 * count :, :] = extra.astype(BF16)


def finish_kernel(part_ref, notes_ref, gain_ref, mail_ref, *outs, act, lane_of):
    _, count, tokens = part_ref.shape
    mine, _, quarter = spot()
    own_gain = upright([gain_ref[...]])[:, 0:1]
    lane = lanes((count, 128))
    sums = notes_ref[0, 2 * count :].astype(F32)
    for place in range(1, 4):
        sums = sums + notes_ref[place, 2 * count :].astype(F32)
    before = jnp.maximum(quarter - 1, 0)
    after = jnp.minimum(quarter + 1, 3)
    for side in range(2):
        rows = slice(side * count, (side + 1) * count)
        notes = [notes_ref[place, rows].astype(F32) for place in range(4)]
        total = jnp.zeros((count, 1), F32)
        squares = jnp.zeros((count, 1), F32)
        for low in range(3):
            one, two = notes[low], notes[low + 1]
            edges = jnp.where(
                lane < W,
                two + pltpu.roll(one, W, 1),
                jnp.where(lane < 2 * W, one + pltpu.roll(two, 128 - W, 1), 0.0),
            )
            total = total + jnp.sum(edges, axis=1, keepdims=True)
            squares = squares + jnp.sum(edges * edges, axis=1, keepdims=True)
        top = pltpu.roll(notes_ref[before, rows].astype(F32), W, 1)
        low = pltpu.roll(notes_ref[after, rows].astype(F32), W, 1)
        part = part_ref[side]
        value = jnp.concatenate(
            [
                part[:, :128] + jnp.where(lane < jnp.where(quarter > 0, W, 0), top, 0.0),
                part[:, tokens - 128 :] + jnp.where(lane >= jnp.where(quarter < 3, 128 - W, 128), low, 0.0),
            ],
            axis=1,
        )
        totals, squared = by_group(total), by_group(squares)
        at = tokens + lane_of
        gain = jnp.where(side == mine, own_gain, mail_ref[:, at : at + 1])
        pieces = []
        for group in range(len(totals)):
            first = (side * len(totals) + group) * 6
            whole = totals[group] + jnp.sum(sums[0:1, first : first + 3], axis=1, keepdims=True)
            whole_squares = squared[group] + jnp.sum(sums[0:1, first + 3 : first + 6], axis=1, keepdims=True)
            span = slice(group * WIDE, (group + 1) * WIDE)
            pieces.append(scaled(value[span], whole, whole_squares, gain[span]))
        result = jnp.concatenate(pieces, axis=0)
        result = (silu(result) if act else result).astype(BF16)
        for copy in range(outs[0].shape[0]):
            outs[0][copy, side] = result
        if not act:
            outs[1][side] = value


def project_kernel(query_ref, key_ref, value_ref, got_ref, full_ref, q_ref, kv_ref, whole_ref, stack_ref):
    inner = query_ref.shape[0]
    side, _, _ = spot()
    for index, ref in enumerate((query_ref, key_ref, value_ref)):
        stack_ref[index * inner : (index + 1) * inner] = ref[...]
    gather_into(full_ref, whole_ref)
    mixed = pair(stack_ref[...], got_ref[: 3 * inner], whole_ref)
    for which in range(2):
        here = side if which == 0 else 1 - side
        q_ref[here] = mixed[which][:inner].astype(BF16)
        for copy in range(kv_ref.shape[0]):
            kv_ref[copy, here] = mixed[which][inner:].astype(BF16)


def attend_kernel(q_ref, pairs_ref, out_ref):
    inner = q_ref.shape[1]
    for head in range(2):
        keys = jnp.concatenate([pairs_ref[place, head, :inner] for place in range(4)], axis=1)
        values = jnp.concatenate([pairs_ref[place, head, inner:] for place in range(4)], axis=1)
        scores = lax.dot_general(
            keys, q_ref[head], (((0,), (0,)), ((), ())), preferred_element_type=F32
        ) * (1.0 / math.sqrt(HEAD_DIM))
        raised = jnp.exp(scores - jnp.max(scores, axis=0, keepdims=True))
        weights = (raised * (1.0 / jnp.sum(raised, axis=0, keepdims=True))).astype(BF16)
        mixed = jnp.dot(values, weights, preferred_element_type=F32).astype(BF16)
        for copy in range(out_ref.shape[0]):
            out_ref[copy, head] = mixed


def leave_kernel(weight_ref, got_ref, full_ref, hidden_ref, keep_ref, send_ref, whole_ref, *, at):
    count, depth = weight_ref.shape
    side, _, _ = spot()
    gather_into(full_ref, whole_ref)
    mine, theirs = pair(weight_ref[...], got_ref[at : at + count, :depth], whole_ref)
    keep_ref[...] = (hidden_ref[side] + mine).astype(BF16)
    send_ref[...] = (hidden_ref[1 - side] + theirs).astype(BF16)


def last_kernel(keep_ref, peer_ref, result_ref):
    span = keep_ref.shape[1]
    side, core, _ = spot()
    part = side ^ core
    for ref, at in ((keep_ref, part), (peer_ref, 1 - part)):
        result_ref[pl.ds(pl.multiple_of(at * span, 16), span), :] = ref[...].astype(F32).T.astype(BF16)


def body(
    latent,
    timestep,
    norm_gain_a,
    conv_weight_a,
    time_weight,
    norm_gain_b,
    conv_weight_b,
    norm_gain_c,
    w_query,
    w_key,
    w_value,
    w_out,
):
    rows, width, count = latent.shape
    tokens = rows * width
    share = tokens // 2
    chs = lax.axis_size("ch")
    place = lax.axis_index("row")
    image_id = place // 2
    inner = w_query.shape[0]

    def tall(weight):
        return jnp.transpose(weight, (1, 2, 0, 3)).reshape(9 * count, C)

    field = ((2, count, share), F32)
    half_chs = chs // 2
    active = ((half_chs, 2, count, share), BF16)
    note = ((4, 2 * count + 16, 128), BF16)
    whole = pltpu.VMEM((C, share), BF16)

    gain_a, gain_b, gain_c = (gain.reshape(1, count) for gain in (norm_gain_a, norm_gain_b, norm_gain_c))
    own_a, own_b = tall(conv_weight_a), tall(conv_weight_b)
    flat = latent.reshape(tokens, count)
    turned, sums, half_a = call(
        enter_kernel,
        [((count, tokens), F32), ((count, 128), F32), ((9 * count, C // 2), BF16)],
        [VM, FAR],
        [pltpu.SemaphoreType.DMA],
        limit=ENTER_LIMIT,
    )(flat, own_a)
    peer = swapped(sums)
    got_a = from_beside(half_a, each_core=True)
    (spread_a,) = call(first_kernel, [((chs, count, share), BF16)], [VM] * 4)(turned, sums, peer, gain_a)

    full = lax.all_to_all(spread_a, "ch", 0, 0, tiled=True)
    step_value = jnp.sum(jnp.where(jnp.arange(timestep.shape[0]) == image_id, after(timestep, spread_a), 0)).astype(F32)
    half = TDIM // 2
    freqs = jnp.exp(-math.log(10000.0) * jnp.arange(half, dtype=F32) / half)
    angles = step_value * freqs
    sinus = jnp.concatenate([jnp.cos(angles), jnp.sin(angles)])[None, :].astype(BF16)
    (mail,) = call(mail_kernel, [((count, share + 128), F32)], [VM] * 5)(
        time_weight.T, sinus, gain_b, gain_c, after(flat, spread_a)
    )
    mail = crossed(mail)
    got_b = from_beside(after(own_b, spread_a))
    *late, late_out = [after(weight, spread_a) for weight in (w_query, w_key, w_value, w_out)]
    late.append(jnp.pad(late_out, ((0, 0), (0, C - w_out.shape[1]))))
    got_c = from_beside(jnp.concatenate(late, axis=0))
    other_a = swapped(after(got_a, spread_a))

    def conv(full, own, gots, *bases, copied=False):
        held = [pltpu.VMEM(gots[0].shape, BF16)] * 2 + [pltpu.SemaphoreType.DMA((2,))]
        return call(
            functools.partial(conv_kernel, gots=len(gots), copied=copied),
            [field, note],
            [FAR if copied else VM] + [FAR] * len(gots) + [VM] * (2 + len(bases)),
            [whole] + held,
            limit=CONV_LIMIT if copied else 20 * 2**20,
        )(own, *gots, full, mail, *bases)

    def finish(part, notes, gain, act, lane_of, outs):
        return call(
            functools.partial(finish_kernel, act=act, lane_of=lane_of), outs, [VM] * 4
        )(part, notes, gain, mail)

    part_a, note_a = conv(full, own_a, [got_a, other_a], time_weight.T, sinus)
    notes_a = image_collect(note_a)
    (spread_b,) = finish(part_a, notes_a, gain_b, True, 1, [active])
    full_b = column_collect(spread_b)
    (whole_b,) = call(gather_into, [((C, share), BF16)], [VM])(full_b)
    part_b, note_b = conv(whole_b.reshape(chs, count, share), own_b, [got_b], flat, copied=True)
    notes_b = image_collect(note_b)
    spread_c, hidden_b = finish(part_b, notes_b, gain_c, False, 2, [active, field])
    features = column_collect(after(spread_c, got_c))

    query, key_value = call(
        project_kernel,
        [((2, inner, share), BF16), ((4, 2, 2 * inner, share), BF16)],
        [VM] * 5,
        [whole, pltpu.VMEM((3 * inner, C), BF16)],
    )(w_query, w_key, w_value, got_c, features)
    pairs = image_collect(key_value)
    (heads_out,) = call(attend_kernel, [((half_chs, 2, inner, share), BF16)], [VM] * 2)(query, pairs)
    kept, sent = call(
        functools.partial(leave_kernel, at=3 * inner),
        [((count, share), BF16)] * 2,
        [VM] * 4,
        [pltpu.VMEM((w_out.shape[1], share), BF16)],
    )(w_out, got_c, column_collect(heads_out), hidden_b)
    (result,) = call(last_kernel, [((tokens, count), BF16)], [VM] * 2)(kept, crossed(sent))
    return result.reshape(rows, width, count)


def solution(mesh):
    return jax.shard_map(
        body,
        mesh=mesh,
        in_specs=(
            P("row", None, "ch"),
            P(),
            P("ch"),
            P("ch", None, None, None),
            P(None, "ch"),
            P("ch"),
            P("ch", None, None, None),
            P("ch"),
            P("ch", None),
            P("ch", None),
            P("ch", None),
            P("ch", None),
        ),
        out_specs=P("row", None, "ch"),
        check_vma=False,
    )
```
